32 devices in a mesh: row: 4 (over y, x), col: 4 (over z), grp: 2 (over core).
Axes of the slice: x: 2, y: 2, z: 4, core: 2. Of those that a mesh axis runs over, the one named last changes fastest.
Arguments:
- krylov_basis: float32 [30, 8, 8192], P(None, None, 'row'), may hold values from -6 to 6
- lattice: int32 [3, 8192], P(None, 'row'), may hold values from 0 to 95, as said below
- strength_index: int32 [8192], P('row'), may hold values from 0 to 15
- strength_table: float32 [16], replicated, may hold values from 0.05 to 0.4
Outputs:
- new_block: float32 [8, 8192], P(None, 'row')
- hessenberg: float32 [30, 2, 4, 4], replicated
- block_gram: float32 [2, 4, 4], replicated
The draws below stay inside these ranges and needn't reach their ends.
Inputs may be any that keep to these rules, and one draw needn't show every extreme that they name: The 8192 scatterers stand on distinct lattice points.
All inputs are finite; a program needn't handle non-finite values.
Results may differ from the reference program's by a relative error of at most 0.0003.
Values may be sent and summed in bfloat16 or wider, within the bound.
A program may use at most 64 MiB of HBM per device.

```python
import math
import jax
import jax.numpy as jnp
from jax import lax

INC = 4
BASIS = 30
TABLE = 16
GRID = 96
POINTS = 8192


def draw_lattice(key, part):
    cells = jax.random.permutation(key, GRID * GRID * GRID)[:POINTS]
    return jnp.stack([cells // (GRID * GRID), cells // GRID % GRID, cells % GRID]).astype(jnp.int32)


def set_ends(result, rng, smallest, top_value):
    shape = result.shape
    index_at = [jax.random.randint(jax.random.fold_in(rng, axis), (), 0, shape[axis]) for axis in range(len(shape))]
    result = result.at[tuple(index_at)].set(smallest)
    longest = shape.index(max(shape))
    index_at[longest] = (index_at[longest] + 1) % shape[longest]
    return result.at[tuple(index_at)].set(top_value)


def block_scale(key, dims, pieces, least, largest):
    def one(axis_at, parts):
        draws = jax.random.uniform(jax.random.fold_in(jax.random.fold_in(key, 6), axis_at), (parts,), jnp.float32, least / len(pieces), largest / len(pieces))
        return jnp.repeat(jnp.exp(draws), dims[axis_at] // parts).reshape((-1,) + (1,) * (len(dims) - axis_at - 1))

    level = one(*pieces[0])
    for cut in pieces[1:]:
        level = level * one(*cut)
    return level


def bell_draw(rng, dims, width, bound, split=(), kind=jnp.bfloat16):
    gain = block_scale(rng, dims, split, -0.22, 0.18) if split else 1.0
    result = jax.random.normal(rng, dims, jnp.float32) * width * gain
    return jnp.minimum(jnp.maximum(result, -bound), bound).astype(kind)


def setup_inputs(seed: int = 0) -> dict:
    streams_of = jax.random.split(jax.random.key(seed), 5)
    return {
        "krylov_basis": bell_draw(streams_of[0], (BASIS, 2 * INC, POINTS), 1.0, 6.0, ((2, 4),), jnp.float32),
        "lattice": draw_lattice(jax.random.fold_in(streams_of[4], 71), 0),
        "strength_index": set_ends(jax.random.randint(streams_of[2], (POINTS,), 0, TABLE), jax.random.fold_in(streams_of[2], 1), 0, TABLE - 1).astype(jnp.int32),
        "strength_table": jnp.clip(jnp.exp(jax.random.uniform(streams_of[3], (TABLE,), jnp.float32, math.log(0.05), math.log(0.4))), 0.05, 0.4),
    }


wave_number = 2.0
highest = lax.Precision.HIGHEST

def strength_of(strength_table, strength_index):
    matches = strength_index[:, None] == jnp.arange(strength_table.shape[0], dtype=jnp.int32)[None, :]
    return lax.optimization_barrier(jnp.sum(jnp.where(matches, strength_table[None, :], jnp.zeros((), strength_table.dtype)), axis=1))

def green_pair(target, source):
    squared = jnp.zeros((target.shape[1], source.shape[1]), jnp.float32)
    for axis_id in range(3):
        offset = target[axis_id][:, None] - source[axis_id][None, :]
        squared = squared + offset * offset
    distance = jnp.sqrt(jnp.maximum(squared, 1.0))
    phases = wave_number * distance
    inverse = 1.0 / distance
    distinct = squared > 0.5
    real_part = jnp.where(distinct, jnp.cos(phases) * inverse, 0.0)
    imag_part = jnp.where(distinct, jnp.sin(phases) * inverse, 0.0)
    return jnp.concatenate([real_part, imag_part], 0).astype(jnp.bfloat16)

def combine(product, tile_size):
    half_rows = product.shape[0] // 2
    direct = product[:, :tile_size]
    turned = product[:, tile_size:]
    return jnp.concatenate([direct[:half_rows] - turned[half_rows:], direct[half_rows:] + turned[:half_rows]], 0)

def scatter_block(target, source, weighted):
    stacked = green_pair(target, source)
    product = lax.dot_general(weighted, stacked, (((1,), (1,)), ((), ())), preferred_element_type=jnp.float32)
    return combine(product, target.shape[1])

def project(krylov_basis, field):
    return jnp.einsum('jan,bn->jab', krylov_basis, field, precision=highest)

def self_gram(field):
    return jnp.dot(field, field.T, precision=highest)

def complex_parts(gram):
    half_rows = gram.shape[-1] // 2
    real_part = gram[..., :half_rows, :half_rows] + gram[..., half_rows:, half_rows:]
    imag_part = gram[..., :half_rows, half_rows:] - gram[..., half_rows:, :half_rows]
    return (real_part, imag_part)

def subtract(krylov_basis, field, real_part, imag_part):
    upper = jnp.concatenate([real_part, imag_part], -1)
    lower = jnp.concatenate([-imag_part, real_part], -1)
    mixing = jnp.concatenate([upper, lower], -2)
    return field - jnp.einsum('jab,jan->bn', mixing, krylov_basis, precision=highest)

def reference(krylov_basis, lattice, strength_index, strength_table):
    point_total = lattice.shape[1]
    direction = krylov_basis[krylov_basis.shape[0] - 1]
    weighted = (direction * strength_of(strength_table, strength_index)[None, :]).astype(jnp.bfloat16)
    located = lattice.astype(jnp.float32)
    tile_size = math.gcd(point_total, 512)
    targets = located.reshape(3, point_total // tile_size, tile_size).transpose(1, 0, 2)
    tiles = lax.map(lambda target: scatter_block(target, located, weighted), targets)
    scattered = tiles.transpose(1, 0, 2).reshape(direction.shape[0], point_total)
    initial = direction - scattered
    once_real, once_imag = complex_parts(project(krylov_basis, initial) / point_total)
    once = subtract(krylov_basis, initial, once_real, once_imag)
    twice_real, twice_imag = complex_parts(project(krylov_basis, once) / point_total)
    new_block = subtract(krylov_basis, once, twice_real, twice_imag)
    hessenberg = jnp.stack([once_real + twice_real, once_imag + twice_imag], 1)
    norm_real, norm_imag = complex_parts(self_gram(new_block) / point_total)
    block_gram = jnp.stack([norm_real, norm_imag], 0)
    return (new_block, hessenberg, block_gram)
```

```python
import functools
import math

import jax
import jax.numpy as jnp
from jax import lax
from jax.experimental import pallas as pl
from jax.experimental.pallas import tpu as pltpu
from jax.sharding import PartitionSpec as P

SIN = (4.4428408013470655, -7.306699927693229, 3.5893875730482314, -0.7728270191086756)
f32 = jnp.float32
bf16 = jnp.bfloat16
MESH = pl.DeviceIdType.MESH


def poly(u, coefs):
    value = jnp.full_like(u, coefs[-1])
    for c in coefs[-2::-1]:
        value = value * u + c
    return value


def green(squared, masked):
    inverse = lax.rsqrt(squared)
    if masked:
        inverse = jnp.where(squared > 0.5, inverse, 0.0)
    half_turns = squared * inverse * (1.0 / math.pi)
    r = half_turns - jnp.round(half_turns)
    s = r * poly(r * r, SIN)
    twice = s * s
    rest = jnp.maximum(2.0 - twice, 1e-12)
    c = rest * lax.rsqrt(rest)
    real_part = inverse - twice * inverse
    imag_part = s * inverse * c
    return real_part.astype(bf16), imag_part.astype(bf16)


def features(sites, is_source):
    x = sites.astype(f32)
    norm = jnp.sum(x * x, axis=0, keepdims=True)
    high = jnp.floor(norm * (1.0 / 256.0)) * 256.0
    low = norm - high
    one = jnp.ones_like(norm)
    if is_source:
        parts = [-2.0 * x, one, one, high, low, jnp.zeros_like(norm)]
    else:
        parts = [x, high, low, one, one, jnp.zeros_like(norm)]
    return jnp.concatenate(parts, 0)


def split(x):
    high = x.astype(bf16)
    return high, (x - high.astype(f32)).astype(bf16)


def stack(x):
    x_high, x_low = split(x)
    return jnp.concatenate([x_high.astype(f32), x_low.astype(f32)], 0).astype(bf16)


def times_i(x):
    half = x.shape[0] // 2
    return jnp.concatenate([-x[half:], x[:half]], 0)


def fold(x):
    half = x.shape[0] // 2
    return x[:half] + x[half:]


lanes = (((1,), (1,)), ((), ()))


def bit_of(x, size):
    return (x // size) % 2 if isinstance(x, int) else lax.rem(lax.div(x, size), 2)


def xor(a, b, n):
    out = 0
    size = 1
    while size < n:
        out = out + lax.rem(bit_of(a, size) + bit_of(b, size), 2) * size
        size *= 2
    return out


def kernel(
    dims, table_hbm, basis_hbm, lattice_hbm, index_hbm, hess_ref, gram_ref, new_ref,
    table_ref, direction, lattice_ref, index_ref, basis, high, low, tgt, gath,
    overlap, metric, partial, landed, field, near, far,
    copy_sem, *sems,
):
    R, C, G, blk, points, nb, NB, ch, table = dims
    parts = C * G
    T = parts * blk
    K = nb * ch
    half = ch // 2
    KP = NB * ch
    HK = NB * half
    (send_g, recv_g, send_h, recv_h, send_p, recv_p, send_f, recv_f, send_n, recv_n,
     send_z, recv_z) = sems
    row, col, grp = lax.axis_index("row"), lax.axis_index("col"), lax.axis_index("grp")
    me = col * G + grp

    def at(part):
        return pl.ds(pl.multiple_of(part * blk, blk), blk)

    own = at(me)
    loads = [
        pltpu.make_async_copy(lattice_hbm, lattice_ref, copy_sem.at[0]),
        pltpu.make_async_copy(index_hbm.at[:, own], index_ref, copy_sem.at[1]),
        pltpu.make_async_copy(basis_hbm.at[pl.ds(K - ch, ch), own], direction, copy_sem.at[2]),
        pltpu.make_async_copy(table_hbm, table_ref, copy_sem.at[3]),
    ]
    for v in range(T // 128):
        loads.append(pltpu.make_async_copy(
            basis_hbm.at[:, pl.ds(v * 128, 128)], basis.at[v, pl.ds(0, K)], copy_sem.at[4 + v]
        ))
    for load in loads:
        load.start()

    def row_id(other):
        return {"row": other}

    def part_id(other):
        return {"col": lax.div(other, G), "grp": lax.rem(other, G)}

    row_peer = [row] + [xor(row, q, R) for q in range(1, R)]
    part_peer = [me] + [xor(me, s, parts) for s in range(1, parts)]
    barrier = pltpu.get_barrier_semaphore()
    for q in range(1, R):
        pl.semaphore_signal(barrier, inc=1, device_id=row_id(row_peer[q]), device_id_type=MESH)
    for s in range(1, parts):
        pl.semaphore_signal(barrier, inc=1, device_id=part_id(part_peer[s]), device_id_type=MESH)

    def copy_to(src, dst, send, recv, device):
        return pltpu.make_async_remote_copy(
            src_ref=src, dst_ref=dst, send_sem=send, recv_sem=recv, device_id=device,
            device_id_type=MESH,
        )

    basis[:, K:] = jnp.zeros((T // 128, KP - K, 128), f32)
    for load in loads[:4]:
        load.wait()
    index = index_ref[...]
    strength = jnp.zeros(index.shape, f32)
    for entry in range(table):
        strength = jnp.where(index == entry, table_ref[entry], strength)
    own_sites = features(lattice_ref[:, own], True)
    gath[0] = jnp.concatenate([direction[...] * strength, own_sites], 0).astype(bf16)
    zeros = jnp.zeros((8, T), f32)
    tgt[...] = jnp.concatenate([features(lattice_ref[...], False), zeros], 0).astype(bf16)

    def source(slot):
        block = gath[slot].astype(f32)
        sent = block[:ch]
        both = jnp.concatenate([sent, times_i(sent)], 1).astype(bf16)
        sites = jnp.concatenate([block[ch:], jnp.zeros((8, blk), f32)], 0).T.astype(bf16)
        return sites, both

    def pair(src, part, masked=False):
        sites, both = src
        squared = jnp.dot(sites, tgt[:, at(part)], preferred_element_type=f32)
        real_part, imag_part = green(squared, masked)
        return jnp.dot(both, jnp.concatenate([real_part, imag_part], 0), preferred_element_type=f32)

    mine = source(0)
    partial[pl.ds(me, 1)] = pair(mine, me, True)[None]
    for s in range(1, parts):
        partial[pl.ds(part_peer[s], 1)] = pair(mine, part_peer[s])[None]

    pl.semaphore_wait(barrier, R - 1 + parts - 1)
    gathers = [
        copy_to(gath.at[0], gath.at[q], send_g.at[q], recv_g.at[q], row_id(row_peer[q]))
        if q else None for q in range(R)
    ]
    for q in range(R - 1, 0, -1):
        gathers[q].start()

    for load in loads[4:]:
        load.wait()
    overlap[...] = jnp.zeros_like(overlap)
    each = 2

    @pl.loop(0, parts // each)
    def _(i):
        left, right = [], []
        for k in range(each):
            span = at(i * each + k)
            rows = jnp.concatenate(
                [
                    jnp.concatenate(
                        [basis[(i * each + k) * (blk // 128) + v, pl.ds(c, NB, stride=ch), :]
                         for v in range(blk // 128)], 1,
                    )
                    for c in range(ch)
                ], 0,
            )
            b_high, b_low = split(rows)
            high[:, span] = b_high
            low[:, span] = b_low
            left += [b_high, b_high]
            right += [b_high * bf16(0.5), b_low]
        products = lax.dot_general(
            jnp.concatenate(left, 1), jnp.concatenate(right, 1), lanes, preferred_element_type=f32
        )
        overlap[0] += products[:HK, :HK] + products[HK:, HK:]
        overlap[1] += products[:HK, HK:] - products[HK:, :HK]

    even, odd = overlap[0], overlap[1]
    metric[pl.ds(row, 1)] = jnp.concatenate([even + even.T, odd - odd.T], 1)[None]
    for q in range(1, R):
        copy_to(metric.at[row], metric.at[row], send_h.at[q], recv_h.at[row], row_id(row_peer[q])).start()

    for q in range(1, R):
        gathers[q].wait()

    def part_copy(s):
        return copy_to(
            partial.at[part_peer[s]], landed.at[s], send_p.at[s], recv_p.at[s], part_id(part_peer[s])
        )

    def off_row(part, sources):
        total = partial[pl.ds(part, 1)][0]
        for src in sources:
            total = total + pair(src, part)
        return total

    if (R - 1) * parts <= 32:
        sources = [source(q) for q in range(1, R)]
        for s in range(parts - 1, 0, -1):
            partial[pl.ds(part_peer[s], 1)] = off_row(part_peer[s], sources)[None]
            part_copy(s).start()
        total = off_row(me, sources)
    else:
        @pl.loop(0, parts - 1)
        def _(k):
            s = parts - 1 - k
            part = xor(me, s, parts)
            partial[pl.ds(part, 1)] = off_row(part, [source(q) for q in range(1, R)])[None]
            copy_to(partial.at[part], landed.at[s], send_p.at[s], recv_p.at[s], part_id(part)).start()

        total = off_row(me, [source(q) for q in range(1, R)])
    for s in range(parts - 1, 0, -1):
        part_copy(s).wait()
        total = total + landed[s]
    field[:, own] = total

    def field_copy(s, part):
        return copy_to(
            field.at[:, at(part)], field.at[:, at(part)], send_f.at[s], recv_f.at[s],
            part_id(part_peer[s]),
        )


    scale = 1.0 / points
    stacked = stack(total)
    raw = fold(lax.dot_general(
        jnp.concatenate([stacked, stacked], 1), jnp.concatenate([high[:, own], low[:, own]], 1),
        lanes, preferred_element_type=f32,
    ))
    norm = fold(lax.dot_general(stacked, stacked, lanes, preferred_element_type=f32))
    norm = norm[:, :ch] + norm[:, ch:]
    coef = raw[:, :HK] - times_i(raw[:, HK:])
    norm = norm[:, :half] - times_i(norm[:, half:])
    lane = lax.broadcasted_iota(jnp.int32, (ch, HK), 1)
    for a in range(half):
        coef = jnp.where(lane == a * NB + nb, norm[:, a:a + 1], coef)
    near[pl.ds(row, 1)] = coef[None]
    for q in range(R - 1, 0, -1):
        copy_to(near.at[row], near.at[row], send_n.at[q], recv_n.at[row], row_id(row_peer[q])).start()
    for s in range(parts - 1, 0, -1):
        field_copy(s, me).start()

    for q in range(1, R):
        peer = row_peer[q]
        copy_to(metric.at[peer], metric.at[peer], send_h.at[q], recv_h.at[peer], row_id(peer)).wait()
    full = jnp.sum(metric[...], 0) * scale
    full_high, full_low = split(full)
    full_both = jnp.concatenate([full_high, full_low], 0)
    overlap[0], overlap[1] = full[:, :HK], full[:, HK:]
    last = pl.ds(nb - 1, half, stride=NB)
    once = jnp.concatenate([overlap[0, last, :], -overlap[1, last, :]], 0)

    for q in range(1, R):
        peer = row_peer[q]
        copy_to(near.at[peer], near.at[peer], send_n.at[q], recv_n.at[peer], row_id(peer)).wait()
    far[pl.ds(me, 1)] = jnp.sum(near[...], 0)[None]
    for s in range(parts - 1, 0, -1):
        copy_to(far.at[me], far.at[me], send_z.at[s], recv_z.at[me], part_id(part_peer[s])).start()
    for s in range(1, parts):
        field_copy(s, part_peer[s]).wait()
    for s in range(1, parts):
        peer = part_peer[s]
        copy_to(far.at[peer], far.at[peer], send_z.at[s], recv_z.at[peer], part_id(peer)).wait()
    sums = jnp.sum(far[...], 0) * scale

    def apply(x):
        x16 = stack(x)
        y = fold(jnp.dot(jnp.concatenate([x16, x16], 1), full_both, preferred_element_type=f32))
        return y[:, :HK] - times_i(y[:, HK:])

    in_basis = lax.rem(lane, NB) < nb
    at_row = lax.broadcasted_iota(jnp.int32, (ch, HK), 0)
    mixed = jnp.where(in_basis, sums, 0.0)
    once = once - mixed
    both = 2.0 * once - apply(once)
    change = both - jnp.where(lane == at_row * NB + (nb - 1), 1.0, 0.0)
    lifted = stack(jnp.concatenate([change, times_i(change)], 1))
    for part in range(parts):
        cols = slice(part * blk, (part + 1) * blk)
        out = jnp.dot(lifted, high[:, cols], preferred_element_type=f32)
        out = out + jnp.dot(lifted, low[:, cols], preferred_element_type=f32)
        new_ref[:, cols] = -(field[:, cols] + fold(out))
    for i in range(2):
        for a in range(half):
            hess_ref[i, a] = both[i * half:(i + 1) * half, a * NB:a * NB + nb]
    other = mixed + apply(change)
    cross = fold(lax.dot_general(
        stack(jnp.concatenate([change, mixed], 1)), stack(jnp.concatenate([other, change], 1)),
        lanes, preferred_element_type=f32,
    ))
    cross = cross[:, :ch] + cross[:, ch:]
    self_gram = jnp.concatenate([sums[:, a * NB + nb:a * NB + nb + 1] for a in range(half)], 1)
    gram_ref[0] = self_gram[:half].T + cross[:half, :half] + cross[half:, half:]
    gram_ref[1] = self_gram[half:].T + cross[:half, half:] - cross[half:, :half]


def local(krylov_basis, lattice, strength_index, strength_table):
    R, C, G = (lax.axis_size(a) for a in ("row", "col", "grp"))
    nb, ch, T = krylov_basis.shape
    parts = C * G
    blk = T // parts
    K = nb * ch
    half = ch // 2
    NB = -(-(nb + 1) // 32) * 32
    KP, HK = NB * ch, NB * half
    table = strength_table.shape[0]
    dims = (R, C, G, blk, T * R, nb, NB, ch, table)
    vmem = pl.BlockSpec(memory_space=pltpu.VMEM)
    hbm = pl.BlockSpec(memory_space=pltpu.HBM)
    dma = pltpu.SemaphoreType.DMA
    hess, gram, new_block = pl.pallas_call(
        functools.partial(kernel, dims),
        out_shape=(
            jax.ShapeDtypeStruct((2, half, half, nb), f32),
            jax.ShapeDtypeStruct((2, half, half), f32),
            jax.ShapeDtypeStruct((ch, T), f32),
        ),
        in_specs=[hbm, hbm, hbm, hbm],
        out_specs=(vmem, vmem, vmem),
        scratch_shapes=[
            pltpu.SMEM((table,), f32),
            pltpu.VMEM((ch, blk), f32),
            pltpu.VMEM((3, T), jnp.int32),
            pltpu.VMEM((1, blk), jnp.int32),
            pltpu.VMEM((T // 128, KP, 128), f32),
            pltpu.VMEM((KP, T), bf16),
            pltpu.VMEM((KP, T), bf16),
            pltpu.VMEM((16, T), bf16),
            pltpu.VMEM((R, 16, blk), bf16),
            pltpu.VMEM((2, HK, HK), f32),
            pltpu.VMEM((R, HK, 2 * HK), f32),
            pltpu.VMEM((parts, ch, blk), f32),
            pltpu.VMEM((parts, ch, blk), f32),
            pltpu.VMEM((ch, T), f32),
            pltpu.VMEM((R, ch, HK), f32),
            pltpu.VMEM((parts, ch, HK), f32),
            dma((4 + T // 128,)),
            dma((R,)), dma((R,)),
            dma((R,)), dma((R,)),
            dma((parts,)), dma((parts,)),
            dma((parts,)), dma((parts,)),
            dma((R,)), dma((R,)),
            dma((parts,)), dma((parts,)),
        ],
        compiler_params=pltpu.CompilerParams(
            collective_id=0, has_side_effects=True, vmem_limit_bytes=50331648
        ),
        name="foldy_step",
    )(*[pltpu.with_memory_space_constraint(v, pltpu.HBM) for v in (strength_table, krylov_basis.reshape(K, T), lattice, strength_index.reshape(1, T))])
    return (new_block, hess.transpose(3, 0, 1, 2), gram)


def solution(mesh):
    in_specs = (P(None, None, "row"), P(None, "row"), P("row"), P())
    out_specs = (P(None, "row"), P(), P())
    return jax.shard_map(local, mesh=mesh, in_specs=in_specs, out_specs=out_specs, check_vma=False)
```

```python
import functools
import math

import jax
import jax.numpy as jnp
from jax import lax
from jax.experimental import pallas as pl
from jax.experimental.pallas import tpu as pltpu
from jax.sharding import PartitionSpec as P

SIN = (4.442834924970635, -7.306550394807036, 3.5883736565798134, -0.7707881588297861)
f32 = jnp.float32
bf16 = jnp.bfloat16
MESH = pl.DeviceIdType.MESH


def poly(u, coefs):
    value = jnp.full_like(u, coefs[-1])
    for c in coefs[-2::-1]:
        value = value * u + c
    return value


def green(squared, masked):
    inverse = lax.rsqrt(squared)
    if masked:
        inverse = jnp.where(squared > 0.5, inverse, 0.0)
    half_turns = squared * inverse * (1.0 / math.pi)
    r = half_turns - jnp.round(half_turns)
    s = r * poly(r * r, SIN)
    rest = jnp.maximum(2.0 - s * s, 1e-12)
    scaled = rest * inverse
    real_part = scaled - inverse
    imag_part = s * scaled * lax.rsqrt(rest)
    return real_part.astype(bf16), imag_part.astype(bf16)


def features(sites, is_source):
    x = sites.astype(f32)
    norm = jnp.sum(x * x, axis=0, keepdims=True)
    high = jnp.floor(norm * (1.0 / 256.0)) * 256.0
    low = norm - high
    one = jnp.ones_like(norm)
    if is_source:
        parts = [-2.0 * x, one, one, high, low, jnp.zeros_like(norm)]
    else:
        parts = [x, high, low, one, one, jnp.zeros_like(norm)]
    return jnp.concatenate(parts, 0)


def split(x):
    high = x.astype(bf16)
    return high, (x - high.astype(f32)).astype(bf16)


def stack(x):
    x_high, x_low = split(x)
    return jnp.concatenate([x_high.astype(f32), x_low.astype(f32)], 0).astype(bf16)


def times_i(x):
    half = x.shape[0] // 2
    return jnp.concatenate([-x[half:], x[:half]], 0)


def fold(x):
    half = x.shape[0] // 2
    return x[:half] + x[half:]


lanes = (((1,), (1,)), ((), ()))


def bit_of(x, size):
    return (x // size) % 2 if isinstance(x, int) else lax.rem(lax.div(x, size), 2)


def xor(a, b, n):
    out = 0
    size = 1
    while size < n:
        out = out + lax.rem(bit_of(a, size) + bit_of(b, size), 2) * size
        size *= 2
    return out


def position(R, C, G):
    row, col, grp = lax.axis_index("row"), lax.axis_index("col"), lax.axis_index("grp")
    me = col * G + grp
    rows = [row] + [xor(row, q, R) for q in range(1, R)]
    parts = [me] + [xor(me, s, C * G) for s in range(1, C * G)]
    return row, col, grp, me, rows, parts


def copy_to(src, dst, send, recv, device):
    return pltpu.make_async_remote_copy(
        src_ref=src, dst_ref=dst, send_sem=send, recv_sem=recv, device_id=device, device_id_type=MESH
    )


def source(gath, slot):
    block = gath[slot].astype(f32)
    half = block.shape[0] // 2
    sent = block[:half]
    both = jnp.concatenate([sent, times_i(sent)], 1).astype(bf16)
    sites = jnp.concatenate([block[half:], jnp.zeros_like(sent)], 0).T.astype(bf16)
    return sites, both


def pair(src, targets, masked=False):
    sites, both = src
    squared = jnp.dot(sites, targets, preferred_element_type=f32)
    real_part, imag_part = green(squared, masked)
    return jnp.dot(both, jnp.concatenate([real_part, imag_part], 0), preferred_element_type=f32)


def split_rows(basis, i, width, NB, ch):
    rows = jnp.concatenate(
        [
            jnp.concatenate(
                [basis[i * (width // 128) + v, pl.ds(c, NB, stride=ch), :] for v in range(width // 128)], 1
            )
            for c in range(ch)
        ], 0,
    )
    return split(rows)


def first_kernel(
    dims, table_hbm, basis_hbm, lattice_hbm, index_hbm, gath, tgt, partial, high, low, overlap,
    table_ref, direction, lattice_ref, index_ref, basis, copy_sem, send_g, recv_g,
):
    R, C, G, blk, points, nb, NB, ch, table = dims
    parts = C * G
    T = parts * blk
    K = nb * ch
    KP = NB * ch
    HK = KP // 2
    HG = HK // G
    row, col, grp, me, row_peer, part_peer = position(R, C, G)

    def at(part):
        return pl.ds(pl.multiple_of(part * blk, blk), blk)

    own = at(me)
    loads = [
        pltpu.make_async_copy(lattice_hbm, lattice_ref, copy_sem.at[0]),
        pltpu.make_async_copy(index_hbm.at[:, own], index_ref, copy_sem.at[1]),
        pltpu.make_async_copy(basis_hbm.at[pl.ds(K - ch, ch), own], direction, copy_sem.at[2]),
        pltpu.make_async_copy(table_hbm, table_ref, copy_sem.at[3]),
    ]
    for v in range(T // 128):
        loads.append(pltpu.make_async_copy(
            basis_hbm.at[:, pl.ds(v * 128, 128)], basis.at[v, pl.ds(0, K)], copy_sem.at[4 + v]
        ))
    for load in loads:
        load.start()
    barrier = pltpu.get_barrier_semaphore()
    for q in range(1, R):
        pl.semaphore_signal(barrier, inc=1, device_id={"row": row_peer[q]}, device_id_type=MESH)
    basis[:, K:] = jnp.zeros((T // 128, KP - K, 128), f32)
    for load in loads[:4]:
        load.wait()
    index = index_ref[...]
    strength = jnp.zeros(index.shape, f32)
    for entry in range(table):
        strength = jnp.where(index == entry, table_ref[entry], strength)
    own_sites = features(lattice_ref[:, own], True)
    gath[0] = jnp.concatenate([direction[...] * strength, own_sites], 0).astype(bf16)
    pl.semaphore_wait(barrier, R - 1)
    gathers = [None] + [
        copy_to(gath.at[0], gath.at[q], send_g.at[q], recv_g.at[q], {"row": row_peer[q]}) for q in range(1, R)
    ]
    for q in range(R - 1, 0, -1):
        gathers[q].start()
    zeros = jnp.zeros((8, T), f32)
    tgt[...] = jnp.concatenate([features(lattice_ref[...], False), zeros], 0).astype(bf16)
    mine = source(gath, 0)
    for s in range(parts):
        partial[pl.ds(part_peer[s], 1)] = pair(mine, tgt[:, at(part_peer[s])], s == 0)[None]
    for load in loads[4:]:
        load.wait()

    overlap[...] = jnp.zeros_like(overlap)
    real_rows = pl.ds(pl.multiple_of(grp * HG, HG), HG)
    imag_rows = pl.ds(pl.multiple_of(HK + grp * HG, HG), HG)

    @pl.loop(0, parts // 2)
    def _(i):
        left, right = [], []
        for k in range(2):
            cols = at(i * 2 + k)
            b_high, b_low = split_rows(basis, i * 2 + k, blk, NB, ch)
            high[:, cols] = b_high
            low[:, cols] = b_low
            kept = jnp.concatenate([high[real_rows, cols], high[imag_rows, cols]], 0)
            left += [kept, kept]
            right += [b_high * bf16(0.5), b_low]
        products = lax.dot_general(
            jnp.concatenate(left, 1), jnp.concatenate(right, 1), lanes, preferred_element_type=f32
        )
        overlap[0] += products[:HG, :HK] + products[HG:, HK:]
        overlap[1] += products[:HG, HK:] - products[HG:, :HK]

    for q in range(1, R):
        gathers[q].wait()


def kernel(
    dims, gath, tgt, begun, high, low, mine_ref, hess_ref, gram_ref, new_ref,
    overlap, metric, gram, partial, landed, field, near, far, *sems,
):
    R, C, G, blk, points, nb, NB, ch, table = dims
    parts = C * G
    T = parts * blk
    K = nb * ch
    half = ch // 2
    KP = NB * ch
    HK = NB * half
    HG = HK // G
    scale = 1.0 / points
    (send_h, recv_h, send_p, recv_p, send_f, recv_f, send_n, recv_n, send_z, recv_z,
     send_c, recv_c) = sems
    row, col, grp, me, row_peer, part_peer = position(R, C, G)

    def row_id(other):
        return {"row": other}

    def part_id(other):
        return {"col": lax.div(other, G), "grp": lax.rem(other, G)}

    def at(part):
        return pl.ds(pl.multiple_of(part * blk, blk), blk)

    own = at(me)
    barrier = pltpu.get_barrier_semaphore()
    for q in range(1, R):
        pl.semaphore_signal(barrier, inc=1, device_id=row_id(row_peer[q]), device_id_type=MESH)
    for s in range(1, parts):
        pl.semaphore_signal(barrier, inc=1, device_id=part_id(part_peer[s]), device_id_type=MESH)

    def metric_copy(slot, q):
        return copy_to(
            metric.at[slot], metric.at[slot], send_h.at[q], recv_h.at[slot], row_id(row_peer[q])
        )

    def share_copy(slot, k):
        return copy_to(
            gram.at[slot], gram.at[slot], send_c.at[k], recv_c.at[slot], {"grp": lax.rem(grp + k, G)}
        )

    def enter():
        pl.semaphore_wait(barrier, R - 1 + parts - 1)
        metric[pl.ds(row, 1)] = jnp.concatenate([mine_ref[0], mine_ref[1]], 1)[None]
        for q in range(R - 1, 0, -1):
            metric_copy(row, q).start()

    def part_copy(s):
        return copy_to(
            partial.at[part_peer[s]], landed.at[s], send_p.at[s], recv_p.at[s], part_id(part_peer[s])
        )

    def off_row(part, sources):
        total = begun[pl.ds(part, 1)][0]
        for src in sources:
            total = total + pair(src, tgt[:, at(part)])
        return total

    if (R - 1) * parts <= 32:
        sources = [source(gath, q) for q in range(1, R)]
        for first, last in ((parts - 1, parts // 2), (parts // 2 - 1, 1)):
            for s in range(first, last - 1, -1):
                partial[pl.ds(part_peer[s], 1)] = off_row(part_peer[s], sources)[None]
            if last > 1:
                enter()
            for s in range(first, last - 1, -1):
                part_copy(s).start()
        total = off_row(me, sources)
    else:
        enter()

        @pl.loop(0, parts - 1)
        def _(k):
            s = parts - 1 - k
            part = xor(me, s, parts)
            partial[pl.ds(part, 1)] = off_row(part, [source(gath, q) for q in range(1, R)])[None]
            copy_to(partial.at[part], landed.at[s], send_p.at[s], recv_p.at[s], part_id(part)).start()

        total = off_row(me, [source(gath, q) for q in range(1, R)])
    for s in range(parts - 1, 0, -1):
        part_copy(s).wait()
        total = total + landed[s]
    field[:, own] = total

    def field_copy(s, part):
        return copy_to(
            field.at[:, at(part)], field.at[:, at(part)], send_f.at[s], recv_f.at[s],
            part_id(part_peer[s]),
        )


    stacked = stack(total)
    raw = fold(lax.dot_general(
        jnp.concatenate([stacked, stacked], 1), jnp.concatenate([high[:, own], low[:, own]], 1),
        lanes, preferred_element_type=f32,
    ))
    norm = fold(lax.dot_general(stacked, stacked, lanes, preferred_element_type=f32))
    norm = norm[:, :ch] + norm[:, ch:]
    coef = raw[:, :HK] - times_i(raw[:, HK:])
    norm = norm[:, :half] - times_i(norm[:, half:])
    lane = lax.broadcasted_iota(jnp.int32, (ch, HK), 1)
    for a in range(half):
        coef = jnp.where(lane == a * NB + nb, norm[:, a:a + 1], coef)
    near[pl.ds(row, 1)] = coef[None]
    for q in range(R - 1, 0, -1):
        copy_to(near.at[row], near.at[row], send_n.at[q], recv_n.at[row], row_id(row_peer[q])).start()
    for s in range(parts - 1, 0, -1):
        field_copy(s, me).start()

    for q in range(1, R):
        metric_copy(row_peer[q], q).wait()
    gram[pl.ds(grp, 1)] = (jnp.sum(metric[...], 0) * scale)[None]
    for k in range(1, G):
        share_copy(grp, k).start()
    for q in range(1, R):
        peer = row_peer[q]
        copy_to(near.at[peer], near.at[peer], send_n.at[q], recv_n.at[peer], row_id(peer)).wait()
    far[pl.ds(me, 1)] = jnp.sum(near[...], 0)[None]
    for s in range(parts - 1, 0, -1):
        copy_to(far.at[me], far.at[me], send_z.at[s], recv_z.at[me], part_id(part_peer[s])).start()
    for s in range(1, parts):
        field_copy(s, part_peer[s]).wait()
    for k in range(1, G):
        share_copy(grp, k).wait_send()
        share_copy(lax.rem(grp + G - k, G), k).wait_recv()
    parts_of = jnp.concatenate([gram[k] for k in range(G)], 0)
    even, odd = parts_of[:, :HK], parts_of[:, HK:]
    full = jnp.concatenate([even + even.T, odd - odd.T], 1)
    full_high, full_low = split(full)
    full_both = jnp.concatenate([full_high, full_low], 0)
    overlap[0], overlap[1] = full[:, :HK], full[:, HK:]
    last = pl.ds(nb - 1, half, stride=NB)
    once = jnp.concatenate([overlap[0, last, :], -overlap[1, last, :]], 0)
    for s in range(1, parts):
        peer = part_peer[s]
        copy_to(far.at[peer], far.at[peer], send_z.at[s], recv_z.at[peer], part_id(peer)).wait()
    sums = jnp.sum(far[...], 0) * scale

    def apply(x):
        x16 = stack(x)
        y = fold(jnp.dot(jnp.concatenate([x16, x16], 1), full_both, preferred_element_type=f32))
        return y[:, :HK] - times_i(y[:, HK:])

    in_basis = lax.rem(lane, NB) < nb
    at_row = lax.broadcasted_iota(jnp.int32, (ch, HK), 0)
    mixed = jnp.where(in_basis, sums, 0.0)
    once = once - mixed
    both = 2.0 * once - apply(once)
    change = both - jnp.where(lane == at_row * NB + (nb - 1), 1.0, 0.0)
    lifted = stack(jnp.concatenate([change, times_i(change)], 1))
    for part in range(parts):
        cols = slice(part * blk, (part + 1) * blk)
        out = jnp.dot(lifted, high[:, cols], preferred_element_type=f32)
        out = out + jnp.dot(lifted, low[:, cols], preferred_element_type=f32)
        new_ref[:, cols] = -(field[:, cols] + fold(out))
    for i in range(2):
        for a in range(half):
            hess_ref[i, a] = both[i * half:(i + 1) * half, a * NB:a * NB + nb]
    other = mixed + apply(change)
    cross = fold(lax.dot_general(
        stack(jnp.concatenate([change, mixed], 1)), stack(jnp.concatenate([other, change], 1)),
        lanes, preferred_element_type=f32,
    ))
    cross = cross[:, :ch] + cross[:, ch:]
    self_gram = jnp.concatenate([sums[:, a * NB + nb:a * NB + nb + 1] for a in range(half)], 1)
    gram_ref[0] = self_gram[:half].T + cross[:half, :half] + cross[half:, half:]
    gram_ref[1] = self_gram[half:].T + cross[:half, half:] - cross[half:, :half]


def store(*refs):
    sem = refs[-1]
    copies = [pltpu.make_async_copy(refs[i], refs[3 + i], sem.at[i]) for i in (2, 0, 1)]
    for copy in copies:
        copy.start()
    for copy in copies:
        copy.wait()


def local(krylov_basis, lattice, strength_index, strength_table):
    R, C, G = (lax.axis_size(a) for a in ("row", "col", "grp"))
    nb, ch, T = krylov_basis.shape
    parts = C * G
    blk = T // parts
    K = nb * ch
    half = ch // 2
    NB = -(-(nb + 1) // 32) * 32
    KP, HK = NB * ch, NB * half
    table = strength_table.shape[0]
    dims = (R, C, G, blk, T * R, nb, NB, ch, table)
    vmem = pl.BlockSpec(memory_space=pltpu.VMEM)
    hbm = pl.BlockSpec(memory_space=pltpu.HBM)
    dma = pltpu.SemaphoreType.DMA
    begun = pl.pallas_call(
        functools.partial(first_kernel, dims),
        out_shape=(
            jax.ShapeDtypeStruct((R, 2 * ch, blk), bf16),
            jax.ShapeDtypeStruct((16, T), bf16),
            jax.ShapeDtypeStruct((parts, ch, blk), f32),
            jax.ShapeDtypeStruct((KP, T), bf16),
            jax.ShapeDtypeStruct((KP, T), bf16),
            jax.ShapeDtypeStruct((2, HK // G, HK), f32),
        ),
        in_specs=[hbm, hbm, hbm, hbm],
        out_specs=(vmem,) * 6,
        scratch_shapes=[
            pltpu.SMEM((table,), f32),
            pltpu.VMEM((ch, blk), f32),
            pltpu.VMEM((3, T), jnp.int32),
            pltpu.VMEM((1, blk), jnp.int32),
            pltpu.VMEM((T // 128, KP, 128), f32),
            dma((4 + T // 128,)),
            dma((R,)), dma((R,)),
        ],
        compiler_params=pltpu.CompilerParams(
            collective_id=0, has_side_effects=True, vmem_limit_bytes=25165824
        ),
        name="foldy_begin",
    )(*[pltpu.with_memory_space_constraint(v, pltpu.HBM) for v in (strength_table, krylov_basis.reshape(K, T), lattice, strength_index.reshape(1, T))])
    hess, gram, new_block = pl.pallas_call(
        functools.partial(kernel, dims),
        out_shape=(
            jax.ShapeDtypeStruct((2, half, half, nb), f32),
            jax.ShapeDtypeStruct((2, half, half), f32),
            jax.ShapeDtypeStruct((ch, T), f32),
        ),
        in_specs=[vmem] * 6,
        out_specs=(vmem, vmem, vmem),
        scratch_shapes=[
            pltpu.VMEM((2, HK, HK), f32),
            pltpu.VMEM((R, HK // G, 2 * HK), f32),
            pltpu.VMEM((G, HK // G, 2 * HK), f32),
            pltpu.VMEM((parts, ch, blk), f32),
            pltpu.VMEM((parts, ch, blk), f32),
            pltpu.VMEM((ch, T), f32),
            pltpu.VMEM((R, ch, HK), f32),
            pltpu.VMEM((parts, ch, HK), f32),
            dma((R,)), dma((R,)),
            dma((parts,)), dma((parts,)),
            dma((parts,)), dma((parts,)),
            dma((R,)), dma((R,)),
            dma((parts,)), dma((parts,)),
            dma((G,)), dma((G,)),
        ],
        compiler_params=pltpu.CompilerParams(
            collective_id=1, has_side_effects=True, vmem_limit_bytes=25165824
        ),
        name="foldy_step",
    )(*begun)
    hess, gram, new_block = pl.pallas_call(
        store,
        out_shape=tuple(jax.ShapeDtypeStruct(v.shape, v.dtype) for v in (hess, gram, new_block)),
        in_specs=[vmem, vmem, vmem],
        out_specs=(hbm, hbm, hbm),
        scratch_shapes=[dma((3,))],
        compiler_params=pltpu.CompilerParams(vmem_limit_bytes=1048576),
        name="store",
    )(hess, gram, new_block)
    return (new_block, hess.transpose(3, 0, 1, 2), gram)


def solution(mesh):
    in_specs = (P(None, None, "row"), P(None, "row"), P("row"), P())
    out_specs = (P(None, "row"), P(), P())
    return jax.shard_map(local, mesh=mesh, in_specs=in_specs, out_specs=out_specs, check_vma=False)
```

```python
import functools
import math

import jax
import jax.numpy as jnp
from jax import lax
from jax.experimental import pallas as pl
from jax.experimental.pallas import tpu as pltpu
from jax.sharding import PartitionSpec as P

SIN = (4.442834924970635, -7.306550394807036, 3.5883736565798134, -0.7707881588297861)
f32 = jnp.float32
bf16 = jnp.bfloat16
MESH = pl.DeviceIdType.MESH


def poly(u, coefs):
    value = jnp.full_like(u, coefs[-1])
    for c in coefs[-2::-1]:
        value = value * u + c
    return value


def green(squared, masked):
    inverse = lax.rsqrt(squared)
    if masked:
        inverse = jnp.where(squared > 0.5, inverse, 0.0)
    half_turns = squared * inverse * (1.0 / math.pi)
    r = half_turns - jnp.round(half_turns)
    s = r * poly(r * r, SIN)
    rest = jnp.maximum(2.0 - s * s, 1e-12)
    scaled = rest * inverse
    real_part = scaled - inverse
    imag_part = s * scaled * lax.rsqrt(rest)
    return real_part.astype(bf16), imag_part.astype(bf16)


def features(sites, is_source):
    x = sites.astype(f32)
    norm = jnp.sum(x * x, axis=0, keepdims=True)
    high = jnp.floor(norm * (1.0 / 256.0)) * 256.0
    low = norm - high
    one = jnp.ones_like(norm)
    if is_source:
        parts = [-2.0 * x, one, one, high, low, jnp.zeros_like(norm)]
    else:
        parts = [x, high, low, one, one, jnp.zeros_like(norm)]
    return jnp.concatenate(parts, 0)


def split(x):
    high = x.astype(bf16)
    return high, (x - high.astype(f32)).astype(bf16)


def stack(x):
    x_high, x_low = split(x)
    return jnp.concatenate([x_high.astype(f32), x_low.astype(f32)], 0).astype(bf16)


def times_i(x):
    half = x.shape[0] // 2
    return jnp.concatenate([-x[half:], x[:half]], 0)


def fold(x):
    half = x.shape[0] // 2
    return x[:half] + x[half:]


lanes = (((1,), (1,)), ((), ()))


def bit_of(x, size):
    return (x // size) % 2 if isinstance(x, int) else lax.rem(lax.div(x, size), 2)


def xor(a, b, n):
    out = 0
    size = 1
    while size < n:
        out = out + lax.rem(bit_of(a, size) + bit_of(b, size), 2) * size
        size *= 2
    return out


def position(R, C, G):
    row, col, grp = lax.axis_index("row"), lax.axis_index("col"), lax.axis_index("grp")
    me = col * G + grp
    rows = [row] + [xor(row, q, R) for q in range(1, R)]
    parts = [me] + [xor(me, s, C * G) for s in range(1, C * G)]
    return row, col, grp, me, rows, parts


def copy_to(src, dst, send, recv, device):
    return pltpu.make_async_remote_copy(
        src_ref=src, dst_ref=dst, send_sem=send, recv_sem=recv, device_id=device, device_id_type=MESH
    )


def source(gath, slot):
    block = gath[slot].astype(f32)
    half = block.shape[0] // 2
    sent = block[:half]
    both = jnp.concatenate([sent, times_i(sent)], 1).astype(bf16)
    sites = jnp.concatenate([block[half:], jnp.zeros_like(sent)], 0).T.astype(bf16)
    return sites, both


def pair(src, targets, masked=False):
    sites, both = src
    squared = jnp.dot(sites, targets, preferred_element_type=f32)
    real_part, imag_part = green(squared, masked)
    return jnp.dot(both, jnp.concatenate([real_part, imag_part], 0), preferred_element_type=f32)


def split_rows(basis, i, width, NB, ch):
    rows = jnp.concatenate(
        [
            jnp.concatenate(
                [basis[i * (width // 128) + v, pl.ds(c, NB, stride=ch), :] for v in range(width // 128)], 1
            )
            for c in range(ch)
        ], 0,
    )
    return split(rows)


def first_kernel(
    dims, table_hbm, basis_hbm, lattice_hbm, index_hbm, gath, tgt, partial, high, low, overlap,
    table_ref, direction, lattice_ref, index_ref, basis, copy_sem, send_g, recv_g,
):
    R, C, G, blk, points, nb, NB, ch, table = dims
    parts = C * G
    T = parts * blk
    K = nb * ch
    KP = NB * ch
    HK = KP // 2
    HG = HK // G
    row, col, grp, me, row_peer, part_peer = position(R, C, G)

    def at(part):
        return pl.ds(pl.multiple_of(part * blk, blk), blk)

    own = at(me)
    loads = [
        pltpu.make_async_copy(lattice_hbm, lattice_ref, copy_sem.at[0]),
        pltpu.make_async_copy(index_hbm.at[:, own], index_ref, copy_sem.at[1]),
        pltpu.make_async_copy(basis_hbm.at[pl.ds(K - ch, ch), own], direction, copy_sem.at[2]),
        pltpu.make_async_copy(table_hbm, table_ref, copy_sem.at[3]),
    ]
    for v in range(T // 128):
        loads.append(pltpu.make_async_copy(
            basis_hbm.at[:, pl.ds(v * 128, 128)], basis.at[v, pl.ds(0, K)], copy_sem.at[4 + v]
        ))
    for load in loads:
        load.start()
    barrier = pltpu.get_barrier_semaphore()
    for q in range(1, R):
        pl.semaphore_signal(barrier, inc=1, device_id={"row": row_peer[q]}, device_id_type=MESH)
    basis[:, K:] = jnp.zeros((T // 128, KP - K, 128), f32)
    for load in loads[:4]:
        load.wait()
    index = index_ref[...]
    strength = jnp.zeros(index.shape, f32)
    for entry in range(table):
        strength = jnp.where(index == entry, table_ref[entry], strength)
    own_sites = features(lattice_ref[:, own], True)
    gath[0] = jnp.concatenate([direction[...] * strength, own_sites], 0).astype(bf16)
    pl.semaphore_wait(barrier, R - 1)
    gathers = [None] + [
        copy_to(gath.at[0], gath.at[q], send_g.at[q], recv_g.at[q], {"row": row_peer[q]}) for q in range(1, R)
    ]
    for q in range(R - 1, 0, -1):
        gathers[q].start()
    zeros = jnp.zeros((8, T), f32)
    tgt[...] = jnp.concatenate([features(lattice_ref[...], False), zeros], 0).astype(bf16)
    mine = source(gath, 0)
    for s in range(parts):
        partial[pl.ds(part_peer[s], 1)] = pair(mine, tgt[:, at(part_peer[s])], s == 0)[None]
    for load in loads[4:]:
        load.wait()

    overlap[...] = jnp.zeros_like(overlap)
    real_rows = pl.ds(pl.multiple_of(grp * HG, HG), HG)
    imag_rows = pl.ds(pl.multiple_of(HK + grp * HG, HG), HG)

    @pl.loop(0, parts // 2)
    def _(i):
        left, right = [], []
        for k in range(2):
            cols = at(i * 2 + k)
            b_high, b_low = split_rows(basis, i * 2 + k, blk, NB, ch)
            high[:, cols] = b_high
            low[:, cols] = b_low
            kept = jnp.concatenate([high[real_rows, cols], high[imag_rows, cols]], 0)
            left += [kept, kept]
            right += [b_high * bf16(0.5), b_low]
        products = lax.dot_general(
            jnp.concatenate(left, 1), jnp.concatenate(right, 1), lanes, preferred_element_type=f32
        )
        overlap[0] += products[:HG, :HK] + products[HG:, HK:]
        overlap[1] += products[:HG, HK:] - products[HG:, :HK]

    for q in range(1, R):
        gathers[q].wait()


def kernel(
    dims, gath, tgt, begun, high, low, mine_ref, hess_ref, gram_ref, new_ref,
    overlap, metric, gram, partial, landed, field, near, far, *sems,
):
    R, C, G, blk, points, nb, NB, ch, table = dims
    parts = C * G
    T = parts * blk
    K = nb * ch
    half = ch // 2
    KP = NB * ch
    HK = NB * half
    HG = HK // G
    scale = 1.0 / points
    (send_h, recv_h, send_p, recv_p, send_f, recv_f, send_n, recv_n, send_z, recv_z,
     send_c, recv_c) = sems
    row, col, grp, me, row_peer, part_peer = position(R, C, G)

    def row_id(other):
        return {"row": other}

    def part_id(other):
        return {"col": lax.div(other, G), "grp": lax.rem(other, G)}

    def at(part):
        return pl.ds(pl.multiple_of(part * blk, blk), blk)

    own = at(me)
    core_peer = [grp] + [xor(grp, k, G) for k in range(1, G)]
    col_peer = [col] + [xor(col, z, C) for z in range(1, C)]
    barrier = pltpu.get_barrier_semaphore()
    for q in range(1, R):
        for k in range(G):
            pl.semaphore_signal(
                barrier, inc=1, device_id={"row": row_peer[q], "grp": core_peer[k]}, device_id_type=MESH
            )
    for s in range(1, parts):
        pl.semaphore_signal(barrier, inc=1, device_id=part_id(part_peer[s]), device_id_type=MESH)

    def metric_copy(slot, q):
        return copy_to(
            metric.at[slot], metric.at[slot], send_h.at[q], recv_h.at[slot], row_id(row_peer[q])
        )

    def share_copy(slot, k):
        return copy_to(
            gram.at[slot], gram.at[slot], send_c.at[k], recv_c.at[slot], {"grp": lax.rem(grp + k, G)}
        )

    def enter():
        pl.semaphore_wait(barrier, (R - 1) * G + parts - 1)
        metric[pl.ds(row, 1)] = jnp.concatenate([mine_ref[0], mine_ref[1]], 1)[None]
        for q in range(R - 1, 0, -1):
            metric_copy(row, q).start()

    def part_copy(s):
        return copy_to(
            partial.at[part_peer[s]], landed.at[s], send_p.at[s], recv_p.at[s], part_id(part_peer[s])
        )

    def off_row(part, sources):
        total = begun[pl.ds(part, 1)][0]
        for src in sources:
            total = total + pair(src, tgt[:, at(part)])
        return total

    if (R - 1) * parts <= 32:
        sources = [source(gath, q) for q in range(1, R)]
        for batch, leaving in enumerate((range(parts - 1, parts // 2 - 1, -1), range(parts // 2 - 1, 1, -1), (1,))):
            for s in leaving:
                partial[pl.ds(part_peer[s], 1)] = off_row(part_peer[s], sources)[None]
            if batch == 0:
                enter()
            for s in leaving:
                part_copy(s).start()
        total = off_row(me, sources)
    else:
        enter()

        @pl.loop(0, parts - 1)
        def _(k):
            s = parts - 1 - k
            part = xor(me, s, parts)
            partial[pl.ds(part, 1)] = off_row(part, [source(gath, q) for q in range(1, R)])[None]
            copy_to(partial.at[part], landed.at[s], send_p.at[s], recv_p.at[s], part_id(part)).start()

        total = off_row(me, [source(gath, q) for q in range(1, R)])
    for s in range(parts - 1, 0, -1):
        part_copy(s).wait()
        total = total + landed[s]
    field[:, own] = total

    def field_copy(s, part):
        return copy_to(
            field.at[:, at(part)], field.at[:, at(part)], send_f.at[s], recv_f.at[s],
            part_id(part_peer[s]),
        )


    stacked = stack(total)
    raw = fold(lax.dot_general(
        jnp.concatenate([stacked, stacked], 1), jnp.concatenate([high[:, own], low[:, own]], 1),
        lanes, preferred_element_type=f32,
    ))
    norm = fold(lax.dot_general(stacked, stacked, lanes, preferred_element_type=f32))
    norm = norm[:, :ch] + norm[:, ch:]
    coef = raw[:, :HK] - times_i(raw[:, HK:])
    norm = norm[:, :half] - times_i(norm[:, half:])
    lane = lax.broadcasted_iota(jnp.int32, (ch, HK), 1)
    for a in range(half):
        coef = jnp.where(lane == a * NB + nb, norm[:, a:a + 1], coef)
    plane = [
        (row_peer[q] * G + core_peer[k], {"row": row_peer[q], "grp": core_peer[k]}, q * G + k)
        for q in range(R) for k in range(G)
    ]
    here = row * G + grp
    near[pl.ds(here, 1)] = coef[None]
    for slot, device, index in plane[:0:-1]:
        copy_to(near.at[here], near.at[here], send_n.at[index], recv_n.at[here], device).start()
    for s in range(parts - 1, 0, -1):
        field_copy(s, me).start()

    for q in range(1, R):
        metric_copy(row_peer[q], q).wait()
    gram[pl.ds(grp, 1)] = (jnp.sum(metric[...], 0) * scale)[None]
    for k in range(1, G):
        share_copy(grp, k).start()
    for slot, device, index in plane[1:]:
        copy_to(near.at[slot], near.at[slot], send_n.at[index], recv_n.at[slot], device).wait()
    far[pl.ds(col, 1)] = jnp.sum(near[...], 0)[None]
    for z in range(C - 1, 0, -1):
        copy_to(far.at[col], far.at[col], send_z.at[z], recv_z.at[col], {"col": col_peer[z]}).start()
    for s in range(1, parts):
        field_copy(s, part_peer[s]).wait()
    for k in range(1, G):
        share_copy(grp, k).wait_send()
        share_copy(lax.rem(grp + G - k, G), k).wait_recv()
    parts_of = jnp.concatenate([gram[k] for k in range(G)], 0)
    even, odd = parts_of[:, :HK], parts_of[:, HK:]
    full = jnp.concatenate([even + even.T, odd - odd.T], 1)
    full_high, full_low = split(full)
    full_both = jnp.concatenate([full_high, full_low], 0)
    overlap[0], overlap[1] = full[:, :HK], full[:, HK:]
    last = pl.ds(nb - 1, half, stride=NB)
    once = jnp.concatenate([overlap[0, last, :], -overlap[1, last, :]], 0)
    for z in range(1, C):
        peer = col_peer[z]
        copy_to(far.at[peer], far.at[peer], send_z.at[z], recv_z.at[peer], {"col": peer}).wait()
    sums = jnp.sum(far[...], 0) * scale

    def apply(x):
        x16 = stack(x)
        y = fold(jnp.dot(jnp.concatenate([x16, x16], 1), full_both, preferred_element_type=f32))
        return y[:, :HK] - times_i(y[:, HK:])

    in_basis = lax.rem(lane, NB) < nb
    at_row = lax.broadcasted_iota(jnp.int32, (ch, HK), 0)
    mixed = jnp.where(in_basis, sums, 0.0)
    once = once - mixed
    both = 2.0 * once - apply(once)
    change = both - jnp.where(lane == at_row * NB + (nb - 1), 1.0, 0.0)
    lifted = stack(jnp.concatenate([change, times_i(change)], 1))
    for part in range(parts):
        cols = slice(part * blk, (part + 1) * blk)
        out = jnp.dot(lifted, high[:, cols], preferred_element_type=f32)
        out = out + jnp.dot(lifted, low[:, cols], preferred_element_type=f32)
        new_ref[:, cols] = -(field[:, cols] + fold(out))
    for i in range(2):
        for a in range(half):
            hess_ref[i, a] = both[i * half:(i + 1) * half, a * NB:a * NB + nb]
    other = mixed + apply(change)
    cross = fold(lax.dot_general(
        stack(jnp.concatenate([change, mixed], 1)), stack(jnp.concatenate([other, change], 1)),
        lanes, preferred_element_type=f32,
    ))
    cross = cross[:, :ch] + cross[:, ch:]
    self_gram = jnp.concatenate([sums[:, a * NB + nb:a * NB + nb + 1] for a in range(half)], 1)
    gram_ref[0] = self_gram[:half].T + cross[:half, :half] + cross[half:, half:]
    gram_ref[1] = self_gram[half:].T + cross[:half, half:] - cross[half:, :half]


def store(*refs):
    sem = refs[-1]
    copies = [pltpu.make_async_copy(refs[i], refs[3 + i], sem.at[i]) for i in (2, 0, 1)]
    for copy in copies:
        copy.start()
    for copy in copies:
        copy.wait()


def local(krylov_basis, lattice, strength_index, strength_table):
    R, C, G = (lax.axis_size(a) for a in ("row", "col", "grp"))
    nb, ch, T = krylov_basis.shape
    parts = C * G
    blk = T // parts
    K = nb * ch
    half = ch // 2
    NB = -(-(nb + 1) // 32) * 32
    KP, HK = NB * ch, NB * half
    table = strength_table.shape[0]
    dims = (R, C, G, blk, T * R, nb, NB, ch, table)
    vmem = pl.BlockSpec(memory_space=pltpu.VMEM)
    hbm = pl.BlockSpec(memory_space=pltpu.HBM)
    dma = pltpu.SemaphoreType.DMA
    begun = pl.pallas_call(
        functools.partial(first_kernel, dims),
        out_shape=(
            jax.ShapeDtypeStruct((R, 2 * ch, blk), bf16),
            jax.ShapeDtypeStruct((16, T), bf16),
            jax.ShapeDtypeStruct((parts, ch, blk), f32),
            jax.ShapeDtypeStruct((KP, T), bf16),
            jax.ShapeDtypeStruct((KP, T), bf16),
            jax.ShapeDtypeStruct((2, HK // G, HK), f32),
        ),
        in_specs=[hbm, hbm, hbm, hbm],
        out_specs=(vmem,) * 6,
        scratch_shapes=[
            pltpu.SMEM((table,), f32),
            pltpu.VMEM((ch, blk), f32),
            pltpu.VMEM((3, T), jnp.int32),
            pltpu.VMEM((1, blk), jnp.int32),
            pltpu.VMEM((T // 128, KP, 128), f32),
            dma((4 + T // 128,)),
            dma((R,)), dma((R,)),
        ],
        compiler_params=pltpu.CompilerParams(
            collective_id=0, has_side_effects=True, vmem_limit_bytes=25165824
        ),
        name="foldy_begin",
    )(*[pltpu.with_memory_space_constraint(v, pltpu.HBM) for v in (strength_table, krylov_basis.reshape(K, T), lattice, strength_index.reshape(1, T))])
    hess, gram, new_block = pl.pallas_call(
        functools.partial(kernel, dims),
        out_shape=(
            jax.ShapeDtypeStruct((2, half, half, nb), f32),
            jax.ShapeDtypeStruct((2, half, half), f32),
            jax.ShapeDtypeStruct((ch, T), f32),
        ),
        in_specs=[vmem] * 6,
        out_specs=(vmem, vmem, vmem),
        scratch_shapes=[
            pltpu.VMEM((2, HK, HK), f32),
            pltpu.VMEM((R, HK // G, 2 * HK), f32),
            pltpu.VMEM((G, HK // G, 2 * HK), f32),
            pltpu.VMEM((parts, ch, blk), f32),
            pltpu.VMEM((parts, ch, blk), f32),
            pltpu.VMEM((ch, T), f32),
            pltpu.VMEM((R * G, ch, HK), f32),
            pltpu.VMEM((C, ch, HK), f32),
            dma((R,)), dma((R,)),
            dma((parts,)), dma((parts,)),
            dma((parts,)), dma((parts,)),
            dma((R * G,)), dma((R * G,)),
            dma((C,)), dma((C,)),
            dma((G,)), dma((G,)),
        ],
        compiler_params=pltpu.CompilerParams(
            collective_id=1, has_side_effects=True, vmem_limit_bytes=25165824
        ),
        name="foldy_step",
    )(*begun)
    hess, gram, new_block = pl.pallas_call(
        store,
        out_shape=tuple(jax.ShapeDtypeStruct(v.shape, v.dtype) for v in (hess, gram, new_block)),
        in_specs=[vmem, vmem, vmem],
        out_specs=(hbm, hbm, hbm),
        scratch_shapes=[dma((3,))],
        compiler_params=pltpu.CompilerParams(vmem_limit_bytes=1048576),
        name="store",
    )(hess, gram, new_block)
    return (new_block, hess.transpose(3, 0, 1, 2), gram)


def solution(mesh):
    in_specs = (P(None, None, "row"), P(None, "row"), P("row"), P())
    out_specs = (P(None, "row"), P(), P())
    return jax.shard_map(local, mesh=mesh, in_specs=in_specs, out_specs=out_specs, check_vma=False)
```

```python
import functools
import math

import jax
import jax.numpy as jnp
from jax import lax
from jax.experimental import pallas as pl
from jax.experimental.pallas import tpu as pltpu
from jax.sharding import PartitionSpec as P

SIN = (4.442834924970635, -7.306550394807036, 3.5883736565798134, -0.7707881588297861)
f32 = jnp.float32
bf16 = jnp.bfloat16
MESH = pl.DeviceIdType.MESH


def poly(u, coefs):
    value = jnp.full_like(u, coefs[-1])
    for c in coefs[-2::-1]:
        value = value * u + c
    return value


def green(squared, masked):
    inverse = lax.rsqrt(squared)
    if masked:
        inverse = jnp.where(squared > 0.5, inverse, 0.0)
    half_turns = squared * inverse * (1.0 / math.pi)
    r = half_turns - jnp.round(half_turns)
    s = r * poly(r * r, SIN)
    rest = jnp.maximum(2.0 - s * s, 1e-12)
    scaled = rest * inverse
    real_part = scaled - inverse
    imag_part = s * scaled * lax.rsqrt(rest)
    return real_part.astype(bf16), imag_part.astype(bf16)


def features(sites, is_source):
    x = sites.astype(f32)
    norm = jnp.sum(x * x, axis=0, keepdims=True)
    high = jnp.floor(norm * (1.0 / 256.0)) * 256.0
    low = norm - high
    one = jnp.ones_like(norm)
    if is_source:
        parts = [-2.0 * x, one, one, high, low, jnp.zeros_like(norm)]
    else:
        parts = [x, high, low, one, one, jnp.zeros_like(norm)]
    return jnp.concatenate(parts, 0)


def split(x):
    high = x.astype(bf16)
    return high, (x - high.astype(f32)).astype(bf16)


def stack(x):
    x_high, x_low = split(x)
    return jnp.concatenate([x_high.astype(f32), x_low.astype(f32)], 0).astype(bf16)


def times_i(x):
    half = x.shape[0] // 2
    return jnp.concatenate([-x[half:], x[:half]], 0)


def fold(x):
    half = x.shape[0] // 2
    return x[:half] + x[half:]


lanes = (((1,), (1,)), ((), ()))


def bit_of(x, size):
    return (x // size) % 2 if isinstance(x, int) else lax.rem(lax.div(x, size), 2)


def xor(a, b, n):
    out = 0
    size = 1
    while size < n:
        out = out + lax.rem(bit_of(a, size) + bit_of(b, size), 2) * size
        size *= 2
    return out


def position(R, C, G):
    row, col, grp = lax.axis_index("row"), lax.axis_index("col"), lax.axis_index("grp")
    me = col * G + grp
    rows = [row] + [xor(row, q, R) for q in range(1, R)]
    parts = [me] + [xor(me, s, C * G) for s in range(1, C * G)]
    return row, col, grp, me, rows, parts


def copy_to(src, dst, send, recv, device):
    return pltpu.make_async_remote_copy(
        src_ref=src, dst_ref=dst, send_sem=send, recv_sem=recv, device_id=device, device_id_type=MESH
    )


def source(gath, slot):
    block = gath[slot].astype(f32)
    half = block.shape[0] // 2
    sent = block[:half]
    both = jnp.concatenate([sent, times_i(sent)], 1).astype(bf16)
    sites = jnp.concatenate([block[half:], jnp.zeros_like(sent)], 0).T.astype(bf16)
    return sites, both


def pair(src, targets, masked=False):
    sites, both = src
    squared = jnp.dot(sites, targets, preferred_element_type=f32)
    real_part, imag_part = green(squared, masked)
    return jnp.dot(both, jnp.concatenate([real_part, imag_part], 0), preferred_element_type=f32)


def split_rows(basis, i, width, NB, ch):
    rows = jnp.concatenate(
        [
            jnp.concatenate(
                [basis[i * (width // 128) + v, pl.ds(c, NB, stride=ch), :] for v in range(width // 128)], 1
            )
            for c in range(ch)
        ], 0,
    )
    return split(rows)


def first_kernel(
    dims, table_hbm, basis_hbm, lattice_hbm, index_hbm, gath, tgt, partial, high, low, overlap,
    table_ref, direction, lattice_ref, index_ref, basis, copy_sem, send_g, recv_g,
):
    R, C, G, blk, points, nb, NB, ch, table = dims
    parts = C * G
    T = parts * blk
    K = nb * ch
    KP = NB * ch
    HK = KP // 2
    HG = HK // G
    row, col, grp, me, row_peer, part_peer = position(R, C, G)

    def at(part):
        return pl.ds(pl.multiple_of(part * blk, blk), blk)

    own = at(me)
    loads = [
        pltpu.make_async_copy(lattice_hbm, lattice_ref, copy_sem.at[0]),
        pltpu.make_async_copy(index_hbm.at[:, own], index_ref, copy_sem.at[1]),
        pltpu.make_async_copy(basis_hbm.at[pl.ds(K - ch, ch), own], direction, copy_sem.at[2]),
        pltpu.make_async_copy(table_hbm, table_ref, copy_sem.at[3]),
    ]
    for v in range(T // 128):
        loads.append(pltpu.make_async_copy(
            basis_hbm.at[:, pl.ds(v * 128, 128)], basis.at[v, pl.ds(0, K)], copy_sem.at[4 + v]
        ))
    for load in loads:
        load.start()
    barrier = pltpu.get_barrier_semaphore()
    for q in range(1, R):
        pl.semaphore_signal(barrier, inc=1, device_id={"row": row_peer[q]}, device_id_type=MESH)
    basis[:, K:] = jnp.zeros((T // 128, KP - K, 128), f32)
    for load in loads[:4]:
        load.wait()
    index = index_ref[...]
    strength = jnp.zeros(index.shape, f32)
    for entry in range(table):
        strength = jnp.where(index == entry, table_ref[entry], strength)
    own_sites = features(lattice_ref[:, own], True)
    gath[0] = jnp.concatenate([direction[...] * strength, own_sites], 0).astype(bf16)
    pl.semaphore_wait(barrier, R - 1)
    gathers = [None] + [
        copy_to(gath.at[0], gath.at[q], send_g.at[q], recv_g.at[q], {"row": row_peer[q]}) for q in range(1, R)
    ]
    for q in range(R - 1, 0, -1):
        gathers[q].start()
    zeros = jnp.zeros((8, T), f32)
    tgt[...] = jnp.concatenate([features(lattice_ref[...], False), zeros], 0).astype(bf16)
    mine = source(gath, 0)
    for s in range(parts):
        partial[pl.ds(part_peer[s], 1)] = pair(mine, tgt[:, at(part_peer[s])], s == 0)[None]
    for load in loads[4:]:
        load.wait()

    overlap[...] = jnp.zeros_like(overlap)
    real_rows = pl.ds(pl.multiple_of(grp * HG, HG), HG)
    imag_rows = pl.ds(pl.multiple_of(HK + grp * HG, HG), HG)

    @pl.loop(0, parts // 2)
    def _(i):
        left, right = [], []
        for k in range(2):
            cols = at(i * 2 + k)
            b_high, b_low = split_rows(basis, i * 2 + k, blk, NB, ch)
            high[:, cols] = b_high
            low[:, cols] = b_low
            kept = jnp.concatenate([high[real_rows, cols], high[imag_rows, cols]], 0)
            left += [kept, kept]
            right += [b_high * bf16(0.5), b_low]
        products = lax.dot_general(
            jnp.concatenate(left, 1), jnp.concatenate(right, 1), lanes, preferred_element_type=f32
        )
        overlap[0] += products[:HG, :HK] + products[HG:, HK:]
        overlap[1] += products[:HG, HK:] - products[HG:, :HK]

    for q in range(1, R):
        gathers[q].wait()


def kernel(
    dims, gath, tgt, begun, high, low, mine_ref, sums_ref, once_ref, full_ref, field,
    overlap, metric, gram, partial, landed, near, far, *sems,
):
    R, C, G, blk, points, nb, NB, ch, table = dims
    parts = C * G
    T = parts * blk
    K = nb * ch
    half = ch // 2
    KP = NB * ch
    HK = NB * half
    HG = HK // G
    scale = 1.0 / points
    (send_h, recv_h, send_p, recv_p, send_f, recv_f, send_n, recv_n, send_z, recv_z,
     send_c, recv_c) = sems
    row, col, grp, me, row_peer, part_peer = position(R, C, G)

    def row_id(other):
        return {"row": other}

    def part_id(other):
        return {"col": lax.div(other, G), "grp": lax.rem(other, G)}

    def at(part):
        return pl.ds(pl.multiple_of(part * blk, blk), blk)

    own = at(me)
    core_peer = [grp] + [xor(grp, k, G) for k in range(1, G)]
    col_peer = [col] + [xor(col, z, C) for z in range(1, C)]
    barrier = pltpu.get_barrier_semaphore()
    for q in range(1, R):
        for k in range(G):
            pl.semaphore_signal(
                barrier, inc=1, device_id={"row": row_peer[q], "grp": core_peer[k]}, device_id_type=MESH
            )
    for s in range(1, parts):
        pl.semaphore_signal(barrier, inc=1, device_id=part_id(part_peer[s]), device_id_type=MESH)

    def metric_copy(slot, q):
        return copy_to(
            metric.at[slot], metric.at[slot], send_h.at[q], recv_h.at[slot], row_id(row_peer[q])
        )

    def share_copy(slot, k):
        return copy_to(
            gram.at[slot], gram.at[slot], send_c.at[k], recv_c.at[slot], {"grp": lax.rem(grp + k, G)}
        )

    def enter():
        pl.semaphore_wait(barrier, (R - 1) * G + parts - 1)
        metric[pl.ds(row, 1)] = jnp.concatenate([mine_ref[0], mine_ref[1]], 1)[None]
        for q in range(R - 1, 0, -1):
            metric_copy(row, q).start()

    def part_copy(s):
        return copy_to(
            partial.at[part_peer[s]], landed.at[s], send_p.at[s], recv_p.at[s], part_id(part_peer[s])
        )

    def off_row(part, sources):
        total = begun[pl.ds(part, 1)][0]
        for src in sources:
            total = total + pair(src, tgt[:, at(part)])
        return total

    if (R - 1) * parts <= 32:
        sources = [source(gath, q) for q in range(1, R)]
        for batch, leaving in enumerate((range(parts - 1, parts // 2 - 1, -1), range(parts // 2 - 1, 1, -1), (1,))):
            for s in leaving:
                partial[pl.ds(part_peer[s], 1)] = off_row(part_peer[s], sources)[None]
            if batch == 0:
                enter()
            for s in leaving:
                part_copy(s).start()
        total = off_row(me, sources)
    else:
        enter()

        @pl.loop(0, parts - 1)
        def _(k):
            s = parts - 1 - k
            part = xor(me, s, parts)
            partial[pl.ds(part, 1)] = off_row(part, [source(gath, q) for q in range(1, R)])[None]
            copy_to(partial.at[part], landed.at[s], send_p.at[s], recv_p.at[s], part_id(part)).start()

        total = off_row(me, [source(gath, q) for q in range(1, R)])
    for s in range(parts - 1, 0, -1):
        part_copy(s).wait()
        total = total + landed[s]
    field[:, own] = total

    def field_copy(s, part):
        return copy_to(
            field.at[:, at(part)], field.at[:, at(part)], send_f.at[s], recv_f.at[s],
            part_id(part_peer[s]),
        )


    for s in range(parts - 1, 0, -1):
        field_copy(s, me).start()
    stacked = stack(total)
    raw = fold(lax.dot_general(
        jnp.concatenate([stacked, stacked], 1), jnp.concatenate([high[:, own], low[:, own]], 1),
        lanes, preferred_element_type=f32,
    ))
    norm = fold(lax.dot_general(stacked, stacked, lanes, preferred_element_type=f32))
    norm = norm[:, :ch] + norm[:, ch:]
    coef = raw[:, :HK] - times_i(raw[:, HK:])
    norm = norm[:, :half] - times_i(norm[:, half:])
    lane = lax.broadcasted_iota(jnp.int32, (ch, HK), 1)
    for a in range(half):
        coef = jnp.where(lane == a * NB + nb, norm[:, a:a + 1], coef)
    plane = [
        (row_peer[q] * G + core_peer[k], {"row": row_peer[q], "grp": core_peer[k]}, q * G + k)
        for q in range(R) for k in range(G)
    ]
    here = row * G + grp
    near[pl.ds(here, 1)] = coef[None]
    for slot, device, index in plane[:0:-1]:
        copy_to(near.at[here], near.at[here], send_n.at[index], recv_n.at[here], device).start()

    for q in range(1, R):
        metric_copy(row_peer[q], q).wait()
    gram[pl.ds(grp, 1)] = (jnp.sum(metric[...], 0) * scale)[None]
    for k in range(1, G):
        share_copy(grp, k).start()
    for slot, device, index in plane[1:]:
        copy_to(near.at[slot], near.at[slot], send_n.at[index], recv_n.at[slot], device).wait()
    far[pl.ds(col, 1)] = jnp.sum(near[...], 0)[None]
    for z in range(C - 1, 0, -1):
        copy_to(far.at[col], far.at[col], send_z.at[z], recv_z.at[col], {"col": col_peer[z]}).start()
    for s in range(1, parts):
        field_copy(s, part_peer[s]).wait()
    for k in range(1, G):
        share_copy(grp, k).wait_send()
        share_copy(lax.rem(grp + G - k, G), k).wait_recv()
    parts_of = jnp.concatenate([gram[k] for k in range(G)], 0)
    even, odd = parts_of[:, :HK], parts_of[:, HK:]
    full = jnp.concatenate([even + even.T, odd - odd.T], 1)
    full_high, full_low = split(full)
    full_ref[...] = jnp.concatenate([full_high, full_low], 0)
    overlap[0], overlap[1] = full[:, :HK], full[:, HK:]
    last = pl.ds(nb - 1, half, stride=NB)
    once_ref[...] = jnp.concatenate([overlap[0, last, :], -overlap[1, last, :]], 0)
    for z in range(1, C):
        peer = col_peer[z]
        copy_to(far.at[peer], far.at[peer], send_z.at[z], recv_z.at[peer], {"col": peer}).wait()
    sums_ref[...] = jnp.sum(far[...], 0) * scale


def finish(
    dims, sums_ref, once_ref, full_ref, field, high, low, hess_hbm, gram_hbm, new_hbm,
    hess_ref, gram_ref, new_ref, sem,
):
    R, C, G, blk, points, nb, NB, ch, table = dims
    parts = C * G
    half = ch // 2
    HK = NB * half
    sums, once, full_both = sums_ref[...], once_ref[...], full_ref[...]
    lane = lax.broadcasted_iota(jnp.int32, (ch, HK), 1)
    def apply(x):
        x16 = stack(x)
        y = fold(jnp.dot(jnp.concatenate([x16, x16], 1), full_both, preferred_element_type=f32))
        return y[:, :HK] - times_i(y[:, HK:])

    in_basis = lax.rem(lane, NB) < nb
    at_row = lax.broadcasted_iota(jnp.int32, (ch, HK), 0)
    mixed = jnp.where(in_basis, sums, 0.0)
    once = once - mixed
    both = 2.0 * once - apply(once)
    change = both - jnp.where(lane == at_row * NB + (nb - 1), 1.0, 0.0)
    lifted = stack(jnp.concatenate([change, times_i(change)], 1))
    sent = []

    def put(src, dst):
        sent.append(pltpu.make_async_copy(src, dst, sem.at[len(sent)]))
        sent[-1].start()

    for i in range(2):
        for a in range(half):
            hess_ref[i, a] = both[i * half:(i + 1) * half, a * NB:a * NB + nb]
    self_gram = jnp.concatenate([sums[:, a * NB + nb:a * NB + nb + 1] for a in range(half)], 1)
    for part in range(parts):
        cols = slice(part * blk, (part + 1) * blk)
        out = jnp.dot(lifted, high[:, cols], preferred_element_type=f32)
        out = out + jnp.dot(lifted, low[:, cols], preferred_element_type=f32)
        new_ref[:, cols] = -(field[:, cols] + fold(out))
        if part == 0:
            other = mixed + apply(change)
        if part == 2:
            cross = fold(lax.dot_general(
                stack(jnp.concatenate([change, mixed], 1)), stack(jnp.concatenate([other, change], 1)),
                lanes, preferred_element_type=f32,
            ))
            cross = cross[:, :ch] + cross[:, ch:]
        if part == 3:
            gram_ref[0] = self_gram[:half].T + cross[:half, :half] + cross[half:, half:]
            gram_ref[1] = self_gram[half:].T + cross[:half, half:] - cross[half:, :half]
        if part % 2:
            cols = pl.ds((part - 1) * blk, 2 * blk)
            put(new_ref.at[:, cols], new_hbm.at[:, cols])
        if part == 3:
            put(hess_ref, hess_hbm)
            put(gram_ref, gram_hbm)
    for copy in sent:
        copy.wait()


def local(krylov_basis, lattice, strength_index, strength_table):
    R, C, G = (lax.axis_size(a) for a in ("row", "col", "grp"))
    nb, ch, T = krylov_basis.shape
    parts = C * G
    blk = T // parts
    K = nb * ch
    half = ch // 2
    NB = -(-(nb + 1) // 32) * 32
    KP, HK = NB * ch, NB * half
    table = strength_table.shape[0]
    dims = (R, C, G, blk, T * R, nb, NB, ch, table)
    vmem = pl.BlockSpec(memory_space=pltpu.VMEM)
    hbm = pl.BlockSpec(memory_space=pltpu.HBM)
    dma = pltpu.SemaphoreType.DMA
    begun = pl.pallas_call(
        functools.partial(first_kernel, dims),
        out_shape=(
            jax.ShapeDtypeStruct((R, 2 * ch, blk), bf16),
            jax.ShapeDtypeStruct((16, T), bf16),
            jax.ShapeDtypeStruct((parts, ch, blk), f32),
            jax.ShapeDtypeStruct((KP, T), bf16),
            jax.ShapeDtypeStruct((KP, T), bf16),
            jax.ShapeDtypeStruct((2, HK // G, HK), f32),
        ),
        in_specs=[hbm, hbm, hbm, hbm],
        out_specs=(vmem,) * 6,
        scratch_shapes=[
            pltpu.SMEM((table,), f32),
            pltpu.VMEM((ch, blk), f32),
            pltpu.VMEM((3, T), jnp.int32),
            pltpu.VMEM((1, blk), jnp.int32),
            pltpu.VMEM((T // 128, KP, 128), f32),
            dma((4 + T // 128,)),
            dma((R,)), dma((R,)),
        ],
        compiler_params=pltpu.CompilerParams(
            collective_id=0, has_side_effects=True, vmem_limit_bytes=25165824
        ),
        name="foldy_begin",
    )(*[pltpu.with_memory_space_constraint(v, pltpu.HBM) for v in (strength_table, krylov_basis.reshape(K, T), lattice, strength_index.reshape(1, T))])
    ended = pl.pallas_call(
        functools.partial(kernel, dims),
        out_shape=(
            jax.ShapeDtypeStruct((ch, HK), f32),
            jax.ShapeDtypeStruct((ch, HK), f32),
            jax.ShapeDtypeStruct((2 * HK, 2 * HK), bf16),
            jax.ShapeDtypeStruct((ch, T), f32),
        ),
        in_specs=[vmem] * 6,
        out_specs=(vmem,) * 4,
        scratch_shapes=[
            pltpu.VMEM((2, HK, HK), f32),
            pltpu.VMEM((R, HK // G, 2 * HK), f32),
            pltpu.VMEM((G, HK // G, 2 * HK), f32),
            pltpu.VMEM((parts, ch, blk), f32),
            pltpu.VMEM((parts, ch, blk), f32),
            pltpu.VMEM((R * G, ch, HK), f32),
            pltpu.VMEM((C, ch, HK), f32),
            dma((R,)), dma((R,)),
            dma((parts,)), dma((parts,)),
            dma((parts,)), dma((parts,)),
            dma((R * G,)), dma((R * G,)),
            dma((C,)), dma((C,)),
            dma((G,)), dma((G,)),
        ],
        compiler_params=pltpu.CompilerParams(
            collective_id=1, has_side_effects=True, vmem_limit_bytes=25165824
        ),
        name="foldy_step",
    )(*begun)
    outs = (
        jax.ShapeDtypeStruct((2, half, half, nb), f32),
        jax.ShapeDtypeStruct((2, half, half), f32),
        jax.ShapeDtypeStruct((ch, T), f32),
    )
    hess, gram, new_block = pl.pallas_call(
        functools.partial(finish, dims),
        out_shape=outs,
        in_specs=[vmem] * 6,
        out_specs=(hbm,) * 3,
        scratch_shapes=[pltpu.VMEM(v.shape, v.dtype) for v in outs] + [dma((parts // 2 + 2,))],
        compiler_params=pltpu.CompilerParams(vmem_limit_bytes=8388608),
        name="foldy_end",
    )(*ended, begun[3], begun[4])
    return (new_block, hess.transpose(3, 0, 1, 2), gram)


def solution(mesh):
    in_specs = (P(None, None, "row"), P(None, "row"), P("row"), P())
    out_specs = (P(None, "row"), P(), P())
    return jax.shard_map(local, mesh=mesh, in_specs=in_specs, out_specs=out_specs, check_vma=False)
```

```python
import functools
import math

import jax
import jax.numpy as jnp
from jax import lax
from jax.experimental import pallas as pl
from jax.experimental.pallas import tpu as pltpu
from jax.sharding import PartitionSpec as P

SIN = (4.442834924970635, -7.306550394807036, 3.5883736565798134, -0.7707881588297861)
f32 = jnp.float32
bf16 = jnp.bfloat16
MESH = pl.DeviceIdType.MESH


def poly(u, coefs):
    value = jnp.full_like(u, coefs[-1])
    for c in coefs[-2::-1]:
        value = value * u + c
    return value


def green(squared, masked):
    inverse = lax.rsqrt(squared)
    if masked:
        inverse = jnp.where(squared > 0.5, inverse, 0.0)
    half_turns = squared * inverse * (1.0 / math.pi)
    r = half_turns - jnp.round(half_turns)
    s = r * poly(r * r, SIN)
    rest = jnp.maximum(2.0 - s * s, 1e-12)
    scaled = rest * inverse
    real_part = scaled - inverse
    imag_part = s * scaled * lax.rsqrt(rest)
    return real_part.astype(bf16), imag_part.astype(bf16)


def features(sites, is_source):
    x = sites.astype(f32)
    norm = jnp.sum(x * x, axis=0, keepdims=True)
    high = jnp.floor(norm * (1.0 / 256.0)) * 256.0
    low = norm - high
    one = jnp.ones_like(norm)
    if is_source:
        parts = [-2.0 * x, one, one, high, low, jnp.zeros_like(norm)]
    else:
        parts = [x, high, low, one, one, jnp.zeros_like(norm)]
    return jnp.concatenate(parts, 0)


def split(x):
    high = x.astype(bf16)
    return high, (x - high.astype(f32)).astype(bf16)


def stack(x):
    x_high, x_low = split(x)
    return jnp.concatenate([x_high.astype(f32), x_low.astype(f32)], 0).astype(bf16)


def times_i(x):
    half = x.shape[0] // 2
    return jnp.concatenate([-x[half:], x[:half]], 0)


def fold(x):
    half = x.shape[0] // 2
    return x[:half] + x[half:]


lanes = (((1,), (1,)), ((), ()))


def bit_of(x, size):
    return (x // size) % 2 if isinstance(x, int) else lax.rem(lax.div(x, size), 2)


def xor(a, b, n):
    out = 0
    size = 1
    while size < n:
        out = out + lax.rem(bit_of(a, size) + bit_of(b, size), 2) * size
        size *= 2
    return out


def position(R, C, G):
    row, col, grp = lax.axis_index("row"), lax.axis_index("col"), lax.axis_index("grp")
    me = col * G + grp
    rows = [row] + [xor(row, q, R) for q in range(1, R)]
    parts = [me] + [xor(me, s, C * G) for s in range(1, C * G)]
    return row, col, grp, me, rows, parts


def copy_to(src, dst, send, recv, device):
    return pltpu.make_async_remote_copy(
        src_ref=src, dst_ref=dst, send_sem=send, recv_sem=recv, device_id=device, device_id_type=MESH
    )


def source(gath, slot):
    block = gath[slot].astype(f32)
    half = block.shape[0] // 2
    sent = block[:half]
    both = jnp.concatenate([sent, times_i(sent)], 1).astype(bf16)
    sites = jnp.concatenate([block[half:], jnp.zeros_like(sent)], 0).T.astype(bf16)
    return sites, both


def pair(src, targets, masked=False):
    sites, both = src
    squared = jnp.dot(sites, targets, preferred_element_type=f32)
    real_part, imag_part = green(squared, masked)
    return jnp.dot(both, jnp.concatenate([real_part, imag_part], 0), preferred_element_type=f32)


def split_rows(basis, i, width, NB, ch):
    rows = jnp.concatenate(
        [
            jnp.concatenate(
                [basis[i * (width // 128) + v, pl.ds(c, NB, stride=ch), :] for v in range(width // 128)], 1
            )
            for c in range(ch)
        ], 0,
    )
    return split(rows)


def first_kernel(
    dims, table_hbm, basis_hbm, lattice_hbm, index_hbm, gath, tgt, partial, high, low, overlap,
    table_ref, direction, lattice_ref, index_ref, basis, copy_sem, send_g, recv_g,
):
    R, C, G, blk, points, nb, NB, ch, table = dims
    parts = C * G
    T = parts * blk
    K = nb * ch
    KP = NB * ch
    HK = KP // 2
    HG = HK // G
    row, col, grp, me, row_peer, part_peer = position(R, C, G)

    def at(part):
        return pl.ds(pl.multiple_of(part * blk, blk), blk)

    own = at(me)
    loads = [
        pltpu.make_async_copy(lattice_hbm, lattice_ref, copy_sem.at[0]),
        pltpu.make_async_copy(index_hbm.at[:, own], index_ref, copy_sem.at[1]),
        pltpu.make_async_copy(basis_hbm.at[pl.ds(K - ch, ch), own], direction, copy_sem.at[2]),
        pltpu.make_async_copy(table_hbm, table_ref, copy_sem.at[3]),
    ]
    for v in range(T // 128):
        loads.append(pltpu.make_async_copy(
            basis_hbm.at[:, pl.ds(v * 128, 128)], basis.at[v, pl.ds(0, K)], copy_sem.at[4 + v]
        ))
    for load in loads:
        load.start()
    barrier = pltpu.get_barrier_semaphore()
    for q in range(1, R):
        pl.semaphore_signal(barrier, inc=1, device_id={"row": row_peer[q]}, device_id_type=MESH)
    basis[:, K:] = jnp.zeros((T // 128, KP - K, 128), f32)
    for load in loads[:4]:
        load.wait()
    index = index_ref[...]
    strength = jnp.zeros(index.shape, f32)
    for entry in range(table):
        strength = jnp.where(index == entry, table_ref[entry], strength)
    own_sites = features(lattice_ref[:, own], True)
    gath[0] = jnp.concatenate([direction[...] * strength, own_sites], 0).astype(bf16)
    pl.semaphore_wait(barrier, R - 1)
    gathers = [None] + [
        copy_to(gath.at[0], gath.at[q], send_g.at[q], recv_g.at[q], {"row": row_peer[q]}) for q in range(1, R)
    ]
    for q in range(R - 1, 0, -1):
        gathers[q].start()
    zeros = jnp.zeros((8, T), f32)
    tgt[...] = jnp.concatenate([features(lattice_ref[...], False), zeros], 0).astype(bf16)
    mine = source(gath, 0)
    for s in range(parts):
        partial[pl.ds(part_peer[s], 1)] = pair(mine, tgt[:, at(part_peer[s])], s == 0)[None]
    for load in loads[4:]:
        load.wait()

    real_rows = pl.ds(pl.multiple_of(grp * HG, HG), HG)
    imag_rows = pl.ds(pl.multiple_of(HK + grp * HG, HG), HG)
    each = 4

    def rows_of_gram(i):
        left, right = [], []
        for k in range(each):
            cols = at(i * each + k)
            b_high, b_low = split_rows(basis, i * each + k, blk, NB, ch)
            high[:, cols] = b_high
            low[:, cols] = b_low
            kept = jnp.concatenate([high[real_rows, cols], high[imag_rows, cols]], 0)
            left += [kept, kept]
            right += [b_high * bf16(0.5), b_low]
        products = lax.dot_general(
            jnp.concatenate(left, 1), jnp.concatenate(right, 1), lanes, preferred_element_type=f32
        )
        return products[:HG, :HK] + products[HG:, HK:], products[:HG, HK:] - products[HG:, :HK]

    overlap[...] = jnp.zeros_like(overlap)

    @pl.loop(0, parts // each)
    def _(i):
        even, odd = rows_of_gram(i)
        overlap[0] += even
        overlap[1] += odd

    for q in range(1, R):
        gathers[q].wait()


def kernel(
    dims, gath, tgt, begun, high, low, mine_ref, sums_ref, once_ref, full_ref, field,
    overlap, metric, gram, partial, landed, near, far, *sems,
):
    R, C, G, blk, points, nb, NB, ch, table = dims
    parts = C * G
    T = parts * blk
    K = nb * ch
    half = ch // 2
    KP = NB * ch
    HK = NB * half
    HG = HK // G
    scale = 1.0 / points
    (send_h, recv_h, send_p, recv_p, send_f, recv_f, send_n, recv_n, send_z, recv_z,
     send_c, recv_c) = sems
    row, col, grp, me, row_peer, part_peer = position(R, C, G)

    def row_id(other):
        return {"row": other}

    def part_id(other):
        return {"col": lax.div(other, G), "grp": lax.rem(other, G)}

    def at(part):
        return pl.ds(pl.multiple_of(part * blk, blk), blk)

    own = at(me)
    core_peer = [grp] + [xor(grp, k, G) for k in range(1, G)]
    col_peer = [col] + [xor(col, z, C) for z in range(1, C)]
    barrier = pltpu.get_barrier_semaphore()
    for q in range(1, R):
        for k in range(G):
            pl.semaphore_signal(
                barrier, inc=1, device_id={"row": row_peer[q], "grp": core_peer[k]}, device_id_type=MESH
            )
    for s in range(1, parts):
        pl.semaphore_signal(barrier, inc=1, device_id=part_id(part_peer[s]), device_id_type=MESH)

    def metric_copy(slot, q):
        return copy_to(
            metric.at[slot], metric.at[slot], send_h.at[q], recv_h.at[slot], row_id(row_peer[q])
        )

    def share_copy(slot, k):
        return copy_to(
            gram.at[slot], gram.at[slot], send_c.at[k], recv_c.at[slot], {"grp": lax.rem(grp + k, G)}
        )

    def enter():
        pl.semaphore_wait(barrier, (R - 1) * G + parts - 1)
        metric[pl.ds(row, 1)] = jnp.concatenate([mine_ref[0], mine_ref[1]], 1)[None]
        for q in range(R - 1, 0, -1):
            metric_copy(row, q).start()

    def part_copy(s):
        return copy_to(
            partial.at[part_peer[s]], landed.at[s], send_p.at[s], recv_p.at[s], part_id(part_peer[s])
        )

    def off_row(part, sources):
        total = begun[pl.ds(part, 1)][0]
        for src in sources:
            total = total + pair(src, tgt[:, at(part)])
        return total

    if (R - 1) * parts <= 32:
        sources = [source(gath, q) for q in range(1, R)]
        for batch, leaving in enumerate((range(parts - 1, parts // 2 - 1, -1), range(parts // 2 - 1, 1, -1), (1,))):
            for s in leaving:
                partial[pl.ds(part_peer[s], 1)] = off_row(part_peer[s], sources)[None]
            if batch == 0:
                enter()
            for s in leaving:
                part_copy(s).start()
        total = off_row(me, sources)
    else:
        enter()

        @pl.loop(0, parts - 1)
        def _(k):
            s = parts - 1 - k
            part = xor(me, s, parts)
            partial[pl.ds(part, 1)] = off_row(part, [source(gath, q) for q in range(1, R)])[None]
            copy_to(partial.at[part], landed.at[s], send_p.at[s], recv_p.at[s], part_id(part)).start()

        total = off_row(me, [source(gath, q) for q in range(1, R)])
    for s in range(parts - 1, 0, -1):
        part_copy(s).wait()
        total = total + landed[s]
    field[:, own] = total

    def field_copy(s, part):
        return copy_to(
            field.at[:, at(part)], field.at[:, at(part)], send_f.at[s], recv_f.at[s],
            part_id(part_peer[s]),
        )


    for s in range(parts - 1, 0, -1):
        field_copy(s, me).start()
    stacked = stack(total)
    raw = fold(lax.dot_general(
        jnp.concatenate([stacked, stacked], 1), jnp.concatenate([high[:, own], low[:, own]], 1),
        lanes, preferred_element_type=f32,
    ))
    norm = fold(lax.dot_general(stacked, stacked, lanes, preferred_element_type=f32))
    norm = norm[:, :ch] + norm[:, ch:]
    coef = raw[:, :HK] - times_i(raw[:, HK:])
    norm = norm[:, :half] - times_i(norm[:, half:])
    lane = lax.broadcasted_iota(jnp.int32, (ch, HK), 1)
    for a in range(half):
        coef = jnp.where(lane == a * NB + nb, norm[:, a:a + 1], coef)
    plane = [
        (row_peer[q] * G + core_peer[k], {"row": row_peer[q], "grp": core_peer[k]}, q * G + k)
        for q in range(R) for k in range(G)
    ]
    here = row * G + grp
    near[pl.ds(here, 1)] = coef[None]
    for slot, device, index in plane[:0:-1]:
        copy_to(near.at[here], near.at[here], send_n.at[index], recv_n.at[here], device).start()

    for q in range(1, R):
        metric_copy(row_peer[q], q).wait()
    gram[pl.ds(grp, 1)] = (jnp.sum(metric[...], 0) * scale)[None]
    for k in range(1, G):
        share_copy(grp, k).start()
    for slot, device, index in plane[1:]:
        copy_to(near.at[slot], near.at[slot], send_n.at[index], recv_n.at[slot], device).wait()
    far[pl.ds(col, 1)] = jnp.sum(near[...], 0)[None]
    for z in range(C - 1, 0, -1):
        copy_to(far.at[col], far.at[col], send_z.at[z], recv_z.at[col], {"col": col_peer[z]}).start()
    for s in range(1, parts):
        field_copy(s, part_peer[s]).wait()
    for k in range(1, G):
        share_copy(grp, k).wait_send()
        share_copy(lax.rem(grp + G - k, G), k).wait_recv()
    parts_of = jnp.concatenate([gram[k] for k in range(G)], 0)
    even, odd = parts_of[:, :HK], parts_of[:, HK:]
    full = jnp.concatenate([even + even.T, odd - odd.T], 1)
    full_high, full_low = split(full)
    full_ref[...] = jnp.concatenate([full_high, full_low], 0)
    overlap[0], overlap[1] = full[:, :HK], full[:, HK:]
    last = pl.ds(nb - 1, half, stride=NB)
    once_ref[...] = jnp.concatenate([overlap[0, last, :], -overlap[1, last, :]], 0)
    for z in range(1, C):
        peer = col_peer[z]
        copy_to(far.at[peer], far.at[peer], send_z.at[z], recv_z.at[peer], {"col": peer}).wait()
    sums_ref[...] = jnp.sum(far[...], 0) * scale


def finish(
    dims, sums_ref, once_ref, full_ref, field, high, low, hess_hbm, gram_hbm, new_hbm,
    hess_ref, gram_ref, new_ref, sem,
):
    R, C, G, blk, points, nb, NB, ch, table = dims
    parts = C * G
    half = ch // 2
    HK = NB * half
    sums, once, full_both = sums_ref[...], once_ref[...], full_ref[...]
    lane = lax.broadcasted_iota(jnp.int32, (ch, HK), 1)
    def apply(x):
        x16 = stack(x)
        y = fold(jnp.dot(jnp.concatenate([x16, x16], 1), full_both, preferred_element_type=f32))
        return y[:, :HK] - times_i(y[:, HK:])

    in_basis = lax.rem(lane, NB) < nb
    at_row = lax.broadcasted_iota(jnp.int32, (ch, HK), 0)
    mixed = jnp.where(in_basis, sums, 0.0)
    once = once - mixed
    both = 2.0 * once - apply(once)
    change = both - jnp.where(lane == at_row * NB + (nb - 1), 1.0, 0.0)
    lifted = stack(jnp.concatenate([change, times_i(change)], 1))
    sent = []

    def put(src, dst):
        sent.append(pltpu.make_async_copy(src, dst, sem.at[len(sent)]))
        sent[-1].start()

    for i in range(2):
        for a in range(half):
            hess_ref[i, a] = both[i * half:(i + 1) * half, a * NB:a * NB + nb]
    self_gram = jnp.concatenate([sums[:, a * NB + nb:a * NB + nb + 1] for a in range(half)], 1)
    for part in range(parts):
        cols = slice(part * blk, (part + 1) * blk)
        out = jnp.dot(lifted, high[:, cols], preferred_element_type=f32)
        out = out + jnp.dot(lifted, low[:, cols], preferred_element_type=f32)
        new_ref[:, cols] = -(field[:, cols] + fold(out))
        if part == 0:
            other = mixed + apply(change)
        if part == 2:
            cross = fold(lax.dot_general(
                stack(jnp.concatenate([change, mixed], 1)), stack(jnp.concatenate([other, change], 1)),
                lanes, preferred_element_type=f32,
            ))
            cross = cross[:, :ch] + cross[:, ch:]
        if part == 3:
            gram_ref[0] = self_gram[:half].T + cross[:half, :half] + cross[half:, half:]
            gram_ref[1] = self_gram[half:].T + cross[:half, half:] - cross[half:, :half]
        if part % 2:
            cols = pl.ds((part - 1) * blk, 2 * blk)
            put(new_ref.at[:, cols], new_hbm.at[:, cols])
        if part == 3:
            put(hess_ref, hess_hbm)
            put(gram_ref, gram_hbm)
    for copy in sent:
        copy.wait()


def local(krylov_basis, lattice, strength_index, strength_table):
    R, C, G = (lax.axis_size(a) for a in ("row", "col", "grp"))
    nb, ch, T = krylov_basis.shape
    parts = C * G
    blk = T // parts
    K = nb * ch
    half = ch // 2
    NB = -(-(nb + 1) // 32) * 32
    KP, HK = NB * ch, NB * half
    table = strength_table.shape[0]
    dims = (R, C, G, blk, T * R, nb, NB, ch, table)
    vmem = pl.BlockSpec(memory_space=pltpu.VMEM)
    hbm = pl.BlockSpec(memory_space=pltpu.HBM)
    dma = pltpu.SemaphoreType.DMA
    begun = pl.pallas_call(
        functools.partial(first_kernel, dims),
        out_shape=(
            jax.ShapeDtypeStruct((R, 2 * ch, blk), bf16),
            jax.ShapeDtypeStruct((16, T), bf16),
            jax.ShapeDtypeStruct((parts, ch, blk), f32),
            jax.ShapeDtypeStruct((KP, T), bf16),
            jax.ShapeDtypeStruct((KP, T), bf16),
            jax.ShapeDtypeStruct((2, HK // G, HK), f32),
        ),
        in_specs=[hbm, hbm, hbm, hbm],
        out_specs=(vmem,) * 6,
        scratch_shapes=[
            pltpu.SMEM((table,), f32),
            pltpu.VMEM((ch, blk), f32),
            pltpu.VMEM((3, T), jnp.int32),
            pltpu.VMEM((1, blk), jnp.int32),
            pltpu.VMEM((T // 128, KP, 128), f32),
            dma((4 + T // 128,)),
            dma((R,)), dma((R,)),
        ],
        compiler_params=pltpu.CompilerParams(
            collective_id=0, has_side_effects=True, vmem_limit_bytes=25165824
        ),
        name="foldy_begin",
    )(*[pltpu.with_memory_space_constraint(v, pltpu.HBM) for v in (strength_table, krylov_basis.reshape(K, T), lattice, strength_index.reshape(1, T))])
    ended = pl.pallas_call(
        functools.partial(kernel, dims),
        out_shape=(
            jax.ShapeDtypeStruct((ch, HK), f32),
            jax.ShapeDtypeStruct((ch, HK), f32),
            jax.ShapeDtypeStruct((2 * HK, 2 * HK), bf16),
            jax.ShapeDtypeStruct((ch, T), f32),
        ),
        in_specs=[vmem] * 6,
        out_specs=(vmem,) * 4,
        scratch_shapes=[
            pltpu.VMEM((2, HK, HK), f32),
            pltpu.VMEM((R, HK // G, 2 * HK), f32),
            pltpu.VMEM((G, HK // G, 2 * HK), f32),
            pltpu.VMEM((parts, ch, blk), f32),
            pltpu.VMEM((parts, ch, blk), f32),
            pltpu.VMEM((R * G, ch, HK), f32),
            pltpu.VMEM((C, ch, HK), f32),
            dma((R,)), dma((R,)),
            dma((parts,)), dma((parts,)),
            dma((parts,)), dma((parts,)),
            dma((R * G,)), dma((R * G,)),
            dma((C,)), dma((C,)),
            dma((G,)), dma((G,)),
        ],
        compiler_params=pltpu.CompilerParams(
            collective_id=1, has_side_effects=True, vmem_limit_bytes=25165824
        ),
        name="foldy_step",
    )(*begun)
    outs = (
        jax.ShapeDtypeStruct((2, half, half, nb), f32),
        jax.ShapeDtypeStruct((2, half, half), f32),
        jax.ShapeDtypeStruct((ch, T), f32),
    )
    hess, gram, new_block = pl.pallas_call(
        functools.partial(finish, dims),
        out_shape=outs,
        in_specs=[vmem] * 6,
        out_specs=(hbm,) * 3,
        scratch_shapes=[pltpu.VMEM(v.shape, v.dtype) for v in outs] + [dma((parts // 2 + 2,))],
        compiler_params=pltpu.CompilerParams(vmem_limit_bytes=8388608),
        name="foldy_end",
    )(*ended, begun[3], begun[4])
    return (new_block, hess.transpose(3, 0, 1, 2), gram)


def solution(mesh):
    in_specs = (P(None, None, "row"), P(None, "row"), P("row"), P())
    out_specs = (P(None, "row"), P(), P())
    return jax.shard_map(local, mesh=mesh, in_specs=in_specs, out_specs=out_specs, check_vma=False)
```

```python
import functools
import math

import jax
import jax.numpy as jnp
from jax import lax
from jax.experimental import pallas as pl
from jax.experimental.pallas import tpu as pltpu
from jax.sharding import PartitionSpec as P

SIN = (4.442834924970635, -7.306550394807036, 3.5883736565798134, -0.7707881588297861)
f32 = jnp.float32
bf16 = jnp.bfloat16
MESH = pl.DeviceIdType.MESH


def poly(u, coefs):
    value = jnp.full_like(u, coefs[-1])
    for c in coefs[-2::-1]:
        value = value * u + c
    return value


def green(squared, masked):
    inverse = lax.rsqrt(squared)
    if masked:
        inverse = jnp.where(squared > 0.5, inverse, 0.0)
    half_turns = squared * inverse * (1.0 / math.pi)
    r = half_turns - jnp.round(half_turns)
    s = r * poly(r * r, SIN)
    rest = jnp.maximum(2.0 - s * s, 1e-12)
    scaled = rest * inverse
    real_part = scaled - inverse
    imag_part = s * scaled * lax.rsqrt(rest)
    return real_part.astype(bf16), imag_part.astype(bf16)


def features(sites, is_source):
    x = sites.astype(f32)
    norm = jnp.sum(x * x, axis=0, keepdims=True)
    high = jnp.floor(norm * (1.0 / 256.0)) * 256.0
    low = norm - high
    one = jnp.ones_like(norm)
    if is_source:
        parts = [-2.0 * x, one, one, high, low, jnp.zeros_like(norm)]
    else:
        parts = [x, high, low, one, one, jnp.zeros_like(norm)]
    return jnp.concatenate(parts, 0)


def split(x):
    high = x.astype(bf16)
    return high, (x - high.astype(f32)).astype(bf16)


def stack(x):
    x_high, x_low = split(x)
    return jnp.concatenate([x_high.astype(f32), x_low.astype(f32)], 0).astype(bf16)


def times_i(x):
    half = x.shape[0] // 2
    return jnp.concatenate([-x[half:], x[:half]], 0)


def fold(x):
    half = x.shape[0] // 2
    return x[:half] + x[half:]


lanes = (((1,), (1,)), ((), ()))


def bit_of(x, size):
    return (x // size) % 2 if isinstance(x, int) else lax.rem(lax.div(x, size), 2)


def xor(a, b, n):
    out = 0
    size = 1
    while size < n:
        out = out + lax.rem(bit_of(a, size) + bit_of(b, size), 2) * size
        size *= 2
    return out


def position(R, C, G):
    row, col, grp = lax.axis_index("row"), lax.axis_index("col"), lax.axis_index("grp")
    me = col * G + grp
    rows = [row] + [xor(row, q, R) for q in range(1, R)]
    parts = [me] + [xor(me, s, C * G) for s in range(1, C * G)]
    return row, col, grp, me, rows, parts


def copy_to(src, dst, send, recv, device):
    return pltpu.make_async_remote_copy(
        src_ref=src, dst_ref=dst, send_sem=send, recv_sem=recv, device_id=device, device_id_type=MESH
    )


def source(gath, slot):
    block = gath[slot].astype(f32)
    half = block.shape[0] // 2
    sent = block[:half]
    both = jnp.concatenate([sent, times_i(sent)], 1).astype(bf16)
    sites = jnp.concatenate([block[half:], jnp.zeros_like(sent)], 0).T.astype(bf16)
    return sites, both


def pair(src, targets, masked=False):
    sites, both = src
    squared = jnp.dot(sites, targets, preferred_element_type=f32)
    real_part, imag_part = green(squared, masked)
    return jnp.dot(both, jnp.concatenate([real_part, imag_part], 0), preferred_element_type=f32)


def split_rows(basis, i, width, NB, ch):
    rows = jnp.concatenate(
        [
            jnp.concatenate(
                [basis[i * (width // 128) + v, pl.ds(c, NB, stride=ch), :] for v in range(width // 128)], 1
            )
            for c in range(ch)
        ], 0,
    )
    return split(rows)


def first_kernel(
    dims, table_hbm, basis_hbm, lattice_hbm, index_hbm, gath, tgt, partial, high, low, overlap,
    table_ref, direction, lattice_ref, index_ref, basis, copy_sem, send_g, recv_g,
):
    R, C, G, blk, points, nb, NB, ch, table = dims
    parts = C * G
    T = parts * blk
    K = nb * ch
    KP = NB * ch
    HK = KP // 2
    HG = HK // G
    row, col, grp, me, row_peer, part_peer = position(R, C, G)

    def at(part):
        return pl.ds(pl.multiple_of(part * blk, blk), blk)

    own = at(me)
    loads = [
        pltpu.make_async_copy(lattice_hbm, lattice_ref, copy_sem.at[0]),
        pltpu.make_async_copy(index_hbm.at[:, own], index_ref, copy_sem.at[1]),
        pltpu.make_async_copy(basis_hbm.at[pl.ds(K - ch, ch), own], direction, copy_sem.at[2]),
        pltpu.make_async_copy(table_hbm, table_ref, copy_sem.at[3]),
    ]
    for v in range(T // 128):
        loads.append(pltpu.make_async_copy(
            basis_hbm.at[:, pl.ds(v * 128, 128)], basis.at[v, pl.ds(0, K)], copy_sem.at[4 + v]
        ))
    for load in loads:
        load.start()
    barrier = pltpu.get_barrier_semaphore()
    for q in range(1, R):
        pl.semaphore_signal(barrier, inc=1, device_id={"row": row_peer[q]}, device_id_type=MESH)
    basis[:, K:] = jnp.zeros((T // 128, KP - K, 128), f32)
    for load in loads[:4]:
        load.wait()
    index = index_ref[...]
    strength = jnp.zeros(index.shape, f32)
    for entry in range(table):
        strength = jnp.where(index == entry, table_ref[entry], strength)
    own_sites = features(lattice_ref[:, own], True)
    gath[0] = jnp.concatenate([direction[...] * strength, own_sites], 0).astype(bf16)
    pl.semaphore_wait(barrier, R - 1)
    gathers = [None] + [
        copy_to(gath.at[0], gath.at[q], send_g.at[q], recv_g.at[q], {"row": row_peer[q]}) for q in range(1, R)
    ]
    for q in range(R - 1, 0, -1):
        gathers[q].start()
    zeros = jnp.zeros((8, T), f32)
    tgt[...] = jnp.concatenate([features(lattice_ref[...], False), zeros], 0).astype(bf16)
    mine = source(gath, 0)
    for s in range(parts):
        partial[pl.ds(part_peer[s], 1)] = pair(mine, tgt[:, at(part_peer[s])], s == 0)[None]
    for load in loads[4:]:
        load.wait()

    real_rows = pl.ds(pl.multiple_of(grp * HG, HG), HG)
    imag_rows = pl.ds(pl.multiple_of(HK + grp * HG, HG), HG)
    each = 4

    def rows_of_gram(i):
        left, right = [], []
        for k in range(each):
            cols = at(i * each + k)
            b_high, b_low = split_rows(basis, i * each + k, blk, NB, ch)
            high[:, cols] = b_high
            low[:, cols] = b_low
            kept = jnp.concatenate([high[real_rows, cols], high[imag_rows, cols]], 0)
            left += [kept, kept]
            right += [b_high * bf16(0.5), b_low]
        products = lax.dot_general(
            jnp.concatenate(left, 1), jnp.concatenate(right, 1), lanes, preferred_element_type=f32
        )
        return products[:HG, :HK] + products[HG:, HK:], products[:HG, HK:] - products[HG:, :HK]

    overlap[...] = jnp.zeros_like(overlap)

    @pl.loop(0, parts // each)
    def _(i):
        even, odd = rows_of_gram(i)
        overlap[0] += even
        overlap[1] += odd

    for q in range(1, R):
        gathers[q].wait()


def kernel(
    dims, gath, tgt, begun, high, low, mine_ref, sums_ref, once_ref, full_ref, field,
    overlap, metric, gram, partial, landed, near, far, *sems,
):
    R, C, G, blk, points, nb, NB, ch, table = dims
    parts = C * G
    T = parts * blk
    K = nb * ch
    half = ch // 2
    KP = NB * ch
    HK = NB * half
    HG = HK // G
    scale = 1.0 / points
    (send_h, recv_h, send_p, recv_p, send_f, recv_f, send_n, recv_n, send_z, recv_z,
     send_c, recv_c) = sems
    row, col, grp, me, row_peer, part_peer = position(R, C, G)

    def row_id(other):
        return {"row": other}

    def part_id(other):
        return {"col": lax.div(other, G), "grp": lax.rem(other, G)}

    def at(part):
        return pl.ds(pl.multiple_of(part * blk, blk), blk)

    own = at(me)
    core_peer = [grp] + [xor(grp, k, G) for k in range(1, G)]
    col_peer = [col] + [xor(col, z, C) for z in range(1, C)]
    barrier = pltpu.get_barrier_semaphore()
    for q in range(1, R):
        for k in range(G):
            pl.semaphore_signal(
                barrier, inc=1, device_id={"row": row_peer[q], "grp": core_peer[k]}, device_id_type=MESH
            )
    for s in range(1, parts):
        pl.semaphore_signal(barrier, inc=1, device_id=part_id(part_peer[s]), device_id_type=MESH)

    def metric_copy(slot, q):
        return copy_to(
            metric.at[slot], metric.at[slot], send_h.at[q], recv_h.at[slot], row_id(row_peer[q])
        )

    def share_copy(slot, k):
        return copy_to(
            gram.at[slot], gram.at[slot], send_c.at[k], recv_c.at[slot], {"grp": lax.rem(grp + k, G)}
        )

    def enter():
        pl.semaphore_wait(barrier, (R - 1) * G + parts - 1)
        metric[pl.ds(row, 1)] = jnp.concatenate([mine_ref[0], mine_ref[1]], 1)[None]
        for q in range(R - 1, 0, -1):
            metric_copy(row, q).start()

    def part_copy(s):
        return copy_to(
            partial.at[part_peer[s]], landed.at[s], send_p.at[s], recv_p.at[s], part_id(part_peer[s])
        )

    def off_row(part, sources):
        total = begun[pl.ds(part, 1)][0]
        for src in sources:
            total = total + pair(src, tgt[:, at(part)])
        return total

    if (R - 1) * parts <= 32:
        sources = [source(gath, q) for q in range(1, R)]
        for batch, leaving in enumerate((range(parts - 1, parts // 2 - 1, -1), range(parts // 2 - 1, 1, -1), (1,))):
            for s in leaving:
                partial[pl.ds(part_peer[s], 1)] = off_row(part_peer[s], sources)[None]
            if batch == 0:
                enter()
            for s in leaving:
                part_copy(s).start()
        total = off_row(me, sources)
    else:
        enter()

        @pl.loop(0, parts - 1)
        def _(k):
            s = parts - 1 - k
            part = xor(me, s, parts)
            partial[pl.ds(part, 1)] = off_row(part, [source(gath, q) for q in range(1, R)])[None]
            copy_to(partial.at[part], landed.at[s], send_p.at[s], recv_p.at[s], part_id(part)).start()

        total = off_row(me, [source(gath, q) for q in range(1, R)])
    for s in range(parts - 1, 0, -1):
        part_copy(s).wait()
        total = total + landed[s]
    field[:, own] = total

    def field_copy(s, part):
        return copy_to(
            field.at[:, at(part)], field.at[:, at(part)], send_f.at[s], recv_f.at[s],
            part_id(part_peer[s]),
        )


    for s in range(parts - 1, 0, -1):
        field_copy(s, me).start()
    stacked = stack(total)
    raw = fold(lax.dot_general(
        jnp.concatenate([stacked, stacked], 1), jnp.concatenate([high[:, own], low[:, own]], 1),
        lanes, preferred_element_type=f32,
    ))
    norm = fold(lax.dot_general(stacked, stacked, lanes, preferred_element_type=f32))
    norm = norm[:, :ch] + norm[:, ch:]
    coef = raw[:, :HK] - times_i(raw[:, HK:])
    norm = norm[:, :half] - times_i(norm[:, half:])
    lane = lax.broadcasted_iota(jnp.int32, (ch, HK), 1)
    for a in range(half):
        coef = jnp.where(lane == a * NB + nb, norm[:, a:a + 1], coef)
    plane = [
        (row_peer[q] * G + core_peer[k], {"row": row_peer[q], "grp": core_peer[k]}, q * G + k)
        for q in range(R) for k in range(G)
    ]
    here = row * G + grp
    near[pl.ds(here, 1)] = coef[None]
    for slot, device, index in plane[:0:-1]:
        copy_to(near.at[here], near.at[here], send_n.at[index], recv_n.at[here], device).start()

    for slot, device, index in plane[1:]:
        copy_to(near.at[slot], near.at[slot], send_n.at[index], recv_n.at[slot], device).wait()
    far[pl.ds(col, 1)] = jnp.sum(near[...], 0)[None]
    for z in range(C - 1, 0, -1):
        copy_to(far.at[col], far.at[col], send_z.at[z], recv_z.at[col], {"col": col_peer[z]}).start()
    for q in range(1, R):
        metric_copy(row_peer[q], q).wait()
    gram[pl.ds(grp, 1)] = (jnp.sum(metric[...], 0) * scale)[None]
    for k in range(1, G):
        share_copy(grp, k).start()
    for s in range(1, parts):
        field_copy(s, part_peer[s]).wait()
    for k in range(1, G):
        share_copy(grp, k).wait_send()
        share_copy(lax.rem(grp + G - k, G), k).wait_recv()
    parts_of = jnp.concatenate([gram[k] for k in range(G)], 0)
    even, odd = parts_of[:, :HK], parts_of[:, HK:]
    full = jnp.concatenate([even + even.T, odd - odd.T], 1)
    full_high, full_low = split(full)
    full_ref[...] = jnp.concatenate([full_high, full_low], 0)
    overlap[0], overlap[1] = full[:, :HK], full[:, HK:]
    last = pl.ds(nb - 1, half, stride=NB)
    once_ref[...] = jnp.concatenate([overlap[0, last, :], -overlap[1, last, :]], 0)
    for z in range(1, C):
        peer = col_peer[z]
        copy_to(far.at[peer], far.at[peer], send_z.at[z], recv_z.at[peer], {"col": peer}).wait()
    sums_ref[...] = jnp.sum(far[...], 0) * scale


def finish(
    dims, sums_ref, once_ref, full_ref, field, high, low, hess_hbm, gram_hbm, new_hbm,
    hess_ref, gram_ref, new_ref, sem,
):
    R, C, G, blk, points, nb, NB, ch, table = dims
    parts = C * G
    half = ch // 2
    HK = NB * half
    sums, once, full_both = sums_ref[...], once_ref[...], full_ref[...]
    lane = lax.broadcasted_iota(jnp.int32, (ch, HK), 1)
    def apply(x):
        x16 = stack(x)
        y = fold(jnp.dot(jnp.concatenate([x16, x16], 1), full_both, preferred_element_type=f32))
        return y[:, :HK] - times_i(y[:, HK:])

    in_basis = lax.rem(lane, NB) < nb
    at_row = lax.broadcasted_iota(jnp.int32, (ch, HK), 0)
    mixed = jnp.where(in_basis, sums, 0.0)
    once = once - mixed
    both = 2.0 * once - apply(once)
    change = both - jnp.where(lane == at_row * NB + (nb - 1), 1.0, 0.0)
    lifted = stack(jnp.concatenate([change, times_i(change)], 1))
    sent = []

    def put(src, dst):
        sent.append(pltpu.make_async_copy(src, dst, sem.at[len(sent)]))
        sent[-1].start()

    for i in range(2):
        for a in range(half):
            hess_ref[i, a] = both[i * half:(i + 1) * half, a * NB:a * NB + nb]
    self_gram = jnp.concatenate([sums[:, a * NB + nb:a * NB + nb + 1] for a in range(half)], 1)
    for part in range(parts):
        cols = slice(part * blk, (part + 1) * blk)
        out = jnp.dot(lifted, high[:, cols], preferred_element_type=f32)
        out = out + jnp.dot(lifted, low[:, cols], preferred_element_type=f32)
        new_ref[:, cols] = -(field[:, cols] + fold(out))
        if part == 0:
            other = mixed + apply(change)
        if part == 2:
            cross = fold(lax.dot_general(
                stack(jnp.concatenate([change, mixed], 1)), stack(jnp.concatenate([other, change], 1)),
                lanes, preferred_element_type=f32,
            ))
            cross = cross[:, :ch] + cross[:, ch:]
        if part == 3:
            gram_ref[0] = self_gram[:half].T + cross[:half, :half] + cross[half:, half:]
            gram_ref[1] = self_gram[half:].T + cross[:half, half:] - cross[half:, :half]
        if part % 2:
            cols = pl.ds((part - 1) * blk, 2 * blk)
            put(new_ref.at[:, cols], new_hbm.at[:, cols])
        if part == 3:
            put(hess_ref, hess_hbm)
            put(gram_ref, gram_hbm)
    for copy in sent:
        copy.wait()


def local(krylov_basis, lattice, strength_index, strength_table):
    R, C, G = (lax.axis_size(a) for a in ("row", "col", "grp"))
    nb, ch, T = krylov_basis.shape
    parts = C * G
    blk = T // parts
    K = nb * ch
    half = ch // 2
    NB = -(-(nb + 1) // 32) * 32
    KP, HK = NB * ch, NB * half
    table = strength_table.shape[0]
    dims = (R, C, G, blk, T * R, nb, NB, ch, table)
    vmem = pl.BlockSpec(memory_space=pltpu.VMEM)
    hbm = pl.BlockSpec(memory_space=pltpu.HBM)
    dma = pltpu.SemaphoreType.DMA
    begun = pl.pallas_call(
        functools.partial(first_kernel, dims),
        out_shape=(
            jax.ShapeDtypeStruct((R, 2 * ch, blk), bf16),
            jax.ShapeDtypeStruct((16, T), bf16),
            jax.ShapeDtypeStruct((parts, ch, blk), f32),
            jax.ShapeDtypeStruct((KP, T), bf16),
            jax.ShapeDtypeStruct((KP, T), bf16),
            jax.ShapeDtypeStruct((2, HK // G, HK), f32),
        ),
        in_specs=[hbm, hbm, hbm, hbm],
        out_specs=(vmem,) * 6,
        scratch_shapes=[
            pltpu.SMEM((table,), f32),
            pltpu.VMEM((ch, blk), f32),
            pltpu.VMEM((3, T), jnp.int32),
            pltpu.VMEM((1, blk), jnp.int32),
            pltpu.VMEM((T // 128, KP, 128), f32),
            dma((4 + T // 128,)),
            dma((R,)), dma((R,)),
        ],
        compiler_params=pltpu.CompilerParams(
            collective_id=0, has_side_effects=True, vmem_limit_bytes=25165824
        ),
        name="foldy_begin",
    )(*[pltpu.with_memory_space_constraint(v, pltpu.HBM) for v in (strength_table, krylov_basis.reshape(K, T), lattice, strength_index.reshape(1, T))])
    ended = pl.pallas_call(
        functools.partial(kernel, dims),
        out_shape=(
            jax.ShapeDtypeStruct((ch, HK), f32),
            jax.ShapeDtypeStruct((ch, HK), f32),
            jax.ShapeDtypeStruct((2 * HK, 2 * HK), bf16),
            jax.ShapeDtypeStruct((ch, T), f32),
        ),
        in_specs=[vmem] * 6,
        out_specs=(vmem,) * 4,
        scratch_shapes=[
            pltpu.VMEM((2, HK, HK), f32),
            pltpu.VMEM((R, HK // G, 2 * HK), f32),
            pltpu.VMEM((G, HK // G, 2 * HK), f32),
            pltpu.VMEM((parts, ch, blk), f32),
            pltpu.VMEM((parts, ch, blk), f32),
            pltpu.VMEM((R * G, ch, HK), f32),
            pltpu.VMEM((C, ch, HK), f32),
            dma((R,)), dma((R,)),
            dma((parts,)), dma((parts,)),
            dma((parts,)), dma((parts,)),
            dma((R * G,)), dma((R * G,)),
            dma((C,)), dma((C,)),
            dma((G,)), dma((G,)),
        ],
        compiler_params=pltpu.CompilerParams(
            collective_id=1, has_side_effects=True, vmem_limit_bytes=25165824
        ),
        name="foldy_step",
    )(*begun)
    outs = (
        jax.ShapeDtypeStruct((2, half, half, nb), f32),
        jax.ShapeDtypeStruct((2, half, half), f32),
        jax.ShapeDtypeStruct((ch, T), f32),
    )
    hess, gram, new_block = pl.pallas_call(
        functools.partial(finish, dims),
        out_shape=outs,
        in_specs=[vmem] * 6,
        out_specs=(hbm,) * 3,
        scratch_shapes=[pltpu.VMEM(v.shape, v.dtype) for v in outs] + [dma((parts // 2 + 2,))],
        compiler_params=pltpu.CompilerParams(vmem_limit_bytes=8388608),
        name="foldy_end",
    )(*ended, begun[3], begun[4])
    return (new_block, hess.transpose(3, 0, 1, 2), gram)


def solution(mesh):
    in_specs = (P(None, None, "row"), P(None, "row"), P("row"), P())
    out_specs = (P(None, "row"), P(), P())
    return jax.shard_map(local, mesh=mesh, in_specs=in_specs, out_specs=out_specs, check_vma=False)
```
